256 devices in a mesh: groups: 4 (over x, y), shard: 64 (over z, core).
Axes of the slice: x: 2, y: 2, z: 32, core: 2. Of those that a mesh axis runs over, the one named last changes fastest.
The devices are a block of a 4x8x32 slice.
Arguments:
- echoes: float32 [1, 2, 8, 512, 8192], P(None, None, 'groups', 'shard'), parts along dimension 2, may hold values from -6 to 6
- waveform: float32 [2, 8192], replicated, may hold values from -6 to 6
- doppler_taper: float32 [512], replicated, may hold values from 0.3 to 1
- cfar_guard: int32 [8], P('groups'), parts along dimension 0, may hold values from 1 to 4, as said below
- cfar_train: int32 [8], P('groups'), parts along dimension 0, may hold values from 2 to 16
- noise_floor: float32 [8], P('groups'), parts along dimension 0, may hold values from 0.5 to 2
Outputs:
- cfar_ratio: float32 [1, 8, 512, 8192], P(None, 'groups', None, 'shard'), parts along dimension 1
The draws below stay inside these ranges and needn't reach their ends.
There are 4 independent parts, one for each index of `groups`. The reference program is written for one: setup_inputs(seed, part) draws one part's arguments, and reference() takes and returns one part's arrays. A program takes and returns all parts, laid end to end along the dimension named above; an argument that names none is the same for every part. Nothing has to cross between parts.
Inputs may be any that keep to these rules, and one draw needn't show every extreme that they name: In every draw some beam has cfar_guard 4 together with cfar_train 16; no beam has more of either.
All inputs are finite; a program needn't handle non-finite values.
Results may differ from the reference program's by a relative error of at most 0.000075.
Values sent between devices are 32-bit elements; how exact they have to be, the bound alone decides.
A program may use at most 64 MiB of HBM per device.

```python
import math
import jax
import jax.numpy as jnp

NCPI = 1
BEAMS = 2
PULSES = 512
GATES = 8192
GUARD_MAX = 4
TRAIN_MAX = 16
HALO = 20


def cfar_windows(key):
    guard_key = jax.random.fold_in(key, 11)
    train_key = jax.random.fold_in(key, 12)
    pick_key = jax.random.fold_in(key, 13)
    guard_cells = jax.random.randint(guard_key, (BEAMS,), 1, GUARD_MAX + 1)
    train_cells = jax.random.randint(train_key, (BEAMS,), 2, TRAIN_MAX + 1)
    chosen = jax.random.randint(pick_key, (), 0, BEAMS)
    widest = jnp.arange(BEAMS) == chosen
    guard_cells = jnp.where(widest, GUARD_MAX, guard_cells)
    train_cells = jnp.where(widest, TRAIN_MAX, train_cells)
    return (guard_cells.astype(jnp.int32), train_cells.astype(jnp.int32))


def draw_cfar_guard(key, part):
    return cfar_windows(key)[0]


def draw_cfar_train(key, part):
    return cfar_windows(key)[1]


def block_scale(stream_key, dims, pieces, smallest, top_value):
    def one(axis_at, blocks):
        heights = jax.random.uniform(jax.random.fold_in(jax.random.fold_in(stream_key, 6), axis_at), (blocks,), jnp.float32, smallest / len(pieces), top_value / len(pieces))
        return jnp.repeat(jnp.exp(heights), dims[axis_at] // blocks).reshape((-1,) + (1,) * (len(dims) - axis_at - 1))

    level = one(*pieces[0])
    for cut in pieces[1:]:
        level = level * one(*cut)
    return level


def normal_values(stream_key, dims, width, reach, cuts=(), kind=jnp.bfloat16):
    level = block_scale(stream_key, dims, cuts, -0.22, 0.18) if cuts else 1.0
    result = jax.random.normal(stream_key, dims, jnp.float32) * width * level
    return jnp.minimum(jnp.maximum(result, -reach), reach).astype(kind)


def setup_inputs(seed: int = 0, part: int = 0) -> dict:
    key_list = jax.random.split(jax.random.key(seed), 7)
    part_keys = jax.random.split(jax.random.fold_in(key_list[6], part), 7)
    echoes = normal_values(part_keys[0], (NCPI, 2, BEAMS, PULSES, GATES), 1.0, 6.0, ((3, 64),), jnp.float32)
    waveform = normal_values(key_list[1], (2, GATES), 1.0, 6.0, (), jnp.float32)
    doppler_taper = jnp.clip(jnp.exp(jax.random.uniform(key_list[2], (PULSES,), jnp.float32, math.log(0.3), math.log(1.0))), 0.3, 1.0)
    cfar_guard = draw_cfar_guard(jax.random.fold_in(jax.random.fold_in(key_list[6], part), 71), part)
    cfar_train = draw_cfar_train(jax.random.fold_in(jax.random.fold_in(key_list[6], part), 71), part)
    noise_floor = jnp.clip(jnp.exp(jax.random.uniform(part_keys[5], (BEAMS,), jnp.float32, math.log(0.5), math.log(2.0))), 0.5, 2.0)
    return dict(echoes=echoes, waveform=waveform, doppler_taper=doppler_taper, cfar_guard=cfar_guard, cfar_train=cfar_train, noise_floor=noise_floor)


def reference(echoes, waveform, doppler_taper, cfar_guard, cfar_train, noise_floor):
    signal = echoes[:, 0] + 1j * echoes[:, 1]
    spectrum = jnp.fft.fft(signal, axis=-1)
    matched = waveform[0] - 1j * waveform[1]
    compressed = jnp.fft.ifft(spectrum * matched, axis=-1)
    tapered = compressed * doppler_taper[:, None]
    doppler = jnp.fft.fft(tapered, axis=2) / jnp.sqrt(jnp.float32(PULSES))
    power_map = jnp.real(doppler) ** 2 + jnp.imag(doppler) ** 2
    padded = jnp.pad(power_map, ((0, 0), (0, 0), (0, 0), (HALO, HALO)))
    offsets = jnp.arange(1, HALO + 1, dtype=jnp.int32)
    inside = (offsets[None, :] > cfar_guard[:, None]) & (offsets[None, :] <= (cfar_guard + cfar_train)[:, None])
    weights = inside.astype(jnp.float32)
    window_sum = jnp.zeros_like(power_map)
    for offset in range(1, HALO + 1):
        lower = padded[..., HALO - offset:HALO - offset + GATES]
        upper = padded[..., HALO + offset:HALO + offset + GATES]
        window_sum = window_sum + weights[:, offset - 1][None, :, None, None] * (lower + upper)
    noise_mean = window_sum / (2.0 * cfar_train.astype(jnp.float32))[None, :, None, None]
    return power_map / (noise_floor[None, :, None, None] + noise_mean)
```

```python
import functools
import math

import jax
import jax.numpy as jnp
import numpy as np
from jax import lax
from jax.experimental import pallas as pl
from jax.experimental.pallas import tpu as pltpu
from jax.sharding import PartitionSpec as P

MESH = pl.DeviceIdType.MESH
GA = 64
GB = 128
HALO = 20
HOP = 8
F32 = jnp.float32
BF16 = jnp.bfloat16


def split_host(table):
    high = table.astype(np.float32).astype(jnp.bfloat16)
    low = (table - high.astype(np.float64)).astype(np.float32).astype(jnp.bfloat16)
    return high, low


def tables(pulses):
    a = np.arange(GA)
    n = np.arange(GB)
    c = np.concatenate([np.arange(0, GB, 2), np.arange(1, GB, 2)])
    ang_a = 2 * math.pi / GA * (np.outer(a, a) % GA)
    ang_b = 2 * math.pi / GB * (np.outer(n, c) % GB)
    ca, sa = np.cos(ang_a), np.sin(ang_a)
    cb, sb = np.cos(ang_b), np.sin(ang_b)
    fwd_a = np.block([[ca, sa], [-sa, ca]])
    inv_a = np.block([[ca, -sa], [sa, ca]])
    fwd_b = np.block([[cb, -sb], [sb, cb]])
    inv_b = np.block([[cb.T, sb.T], [-sb.T, cb.T]])

    def left(m):
        h, l = split_host(m)
        return np.concatenate([h, h, l], axis=1)

    def right(m):
        h, l = split_host(m)
        return np.concatenate([h, h, l], axis=0)

    ang_t = 2 * math.pi / (GA * GB) * (np.outer(a, n) % (GA * GB))
    radix = pulses // GA
    ang_d = 2 * math.pi / pulses * (np.outer(a, np.arange(radix)) % pulses)
    small = np.zeros((GA, GB))
    small[:, :radix] = np.cos(ang_d)
    small[:, radix : 2 * radix] = np.sin(ang_d)
    twid = np.stack([np.cos(ang_t), np.sin(ang_t), small]).astype(np.float32)
    return (
        np.stack([left(fwd_a), left(inv_a)]),
        np.stack([right(fwd_b), right(inv_b)]),
        twid,
    )


def split(x):
    high = x.astype(BF16)
    return high, (x - high.astype(F32)).astype(BF16)


def dot_left(table, values):
    high, low = split(values)
    return jnp.dot(table, jnp.concatenate([high, low, high], axis=0), preferred_element_type=F32)


def dot_right(values, table):
    high, low = split(values)
    return jnp.dot(jnp.concatenate([high, low, high], axis=1), table, preferred_element_type=F32)


def compress(rows_re, rows_im, fwd_a, inv_a, fwd_b, inv_b, tc, ts, fr, fi):
    count = len(rows_re)
    x = jnp.concatenate(
        [jnp.concatenate(rows_re, axis=1), jnp.concatenate(rows_im, axis=1)], axis=0
    )
    y = dot_left(fwd_a, x)
    parts = []
    for p in range(count):
        yr = y[:GA, p * GB : (p + 1) * GB]
        yi = y[GA:, p * GB : (p + 1) * GB]
        parts.append(jnp.concatenate([yr * tc + yi * ts, yi * tc - yr * ts], axis=1))
    z = dot_right(jnp.concatenate(parts, axis=0), fwd_b)
    parts = []
    for p in range(count):
        zr = z[p * GA : (p + 1) * GA, :GB]
        zi = z[p * GA : (p + 1) * GA, GB:]
        parts.append(jnp.concatenate([zr * fr + zi * fi, zi * fr - zr * fi], axis=1))
    v = dot_right(jnp.concatenate(parts, axis=0), inv_b)
    re, im = [], []
    for p in range(count):
        vr = v[p * GA : (p + 1) * GA, :GB]
        vi = v[p * GA : (p + 1) * GA, GB:]
        re.append(vr * tc - vi * ts)
        im.append(vr * ts + vi * tc)
    return dot_left(
        inv_a,
        jnp.concatenate([jnp.concatenate(re, axis=1), jnp.concatenate(im, axis=1)], axis=0),
    )


def butterfly8(xs):
    r = math.sqrt(0.5)

    def add(u, v):
        return u[0] + v[0], u[1] + v[1]

    def sub(u, v):
        return u[0] - v[0], u[1] - v[1]

    def dft4(q):
        s02, d02 = add(q[0], q[2]), sub(q[0], q[2])
        s13, d13 = add(q[1], q[3]), sub(q[1], q[3])
        turned = (d13[1], -d13[0])
        return [add(s02, s13), add(d02, turned), sub(s02, s13), sub(d02, turned)]

    even, odd = dft4(xs[0::2]), dft4(xs[1::2])
    o1 = ((odd[1][0] + odd[1][1]) * r, (odd[1][1] - odd[1][0]) * r)
    o2 = (odd[2][1], -odd[2][0])
    o3 = ((odd[3][1] - odd[3][0]) * r, -(odd[3][0] + odd[3][1]) * r)
    odd = [odd[0], o1, o2, o3]
    return [add(even[k], odd[k]) for k in range(4)] + [sub(even[k], odd[k]) for k in range(4)]


def doppler_power(rows_re, rows_im, fwd_a, turn):
    count = len(rows_re)
    x = jnp.concatenate(
        [jnp.concatenate(rows_re, axis=1), jnp.concatenate(rows_im, axis=1)], axis=0
    )
    y = dot_left(fwd_a, x)
    terms = []
    for l in range(count):
        yr = y[:GA, l * GB : (l + 1) * GB]
        yi = y[GA:, l * GB : (l + 1) * GB]
        if l == 0:
            terms.append((yr, yi))
        else:
            dc, ds = turn(l)
            terms.append((yr * dc + yi * ds, yi * dc - yr * ds))
    return jnp.concatenate([r * r + i * i for r, i in butterfly8(terms)], axis=0)


def filter_grid(grid):
    turned = grid.T
    top, bottom = turned[:GA], turned[GA:]
    low = lax.broadcasted_iota(jnp.int32, (GA, GB), 1) < GA
    fr = jnp.where(low, top, pltpu.roll(bottom, GA, 1))
    fi = jnp.where(low, pltpu.roll(top, GA, 1), bottom)
    return fr, fi


def bands(guard, train):
    i = lax.broadcasted_iota(jnp.int32, (GB, GB), 0)
    j = lax.broadcasted_iota(jnp.int32, (GB, GB), 1)

    def inside(d):
        return jnp.where((d > guard) & (d <= guard + train), 1.0, 0.0).astype(F32)

    own = inside(jnp.abs(i - j))
    slot = lax.rem(i, 32)
    used = jnp.where(slot < HALO, 1.0, 0.0).astype(F32)
    left = inside(j + HALO - slot) * used
    right = inside(slot + GB - j) * used
    return own, left, right


def pack(power, lo):
    rows = power.shape[0] // 4
    lane = lax.broadcasted_iota(jnp.int32, (rows, GB), 1)
    out = None
    for r in range(4):
        block = power[r * rows : (r + 1) * rows]
        shift = (32 * r - lo) % GB
        moved = pltpu.roll(block, shift, 1) if shift else block
        out = moved if out is None else jnp.where(lane >= 32 * r, moved, out)
    return out


def kernel(
    size,
    echoes,
    waveform,
    taper,
    guard,
    train,
    noise,
    tab_a,
    tab_b,
    twid,
    out,
    x_in,
    w_in,
    ta,
    tb,
    tw,
    x_rows,
    grid,
    filt,
    own,
    recv,
    land,
    dop,
    power,
    halo_out,
    halo_in,
    result,
    in_sem,
    own_sem,
    next_sem,
    recv_sem,
    land_sem,
    hs_sem,
    hr_sem,
    out_sem,
):
    chips = size // 2
    me = lax.axis_index("shard")
    chip = lax.div(me, 2)
    core = lax.rem(me, 2)
    beams = echoes.shape[2]
    pulses = echoes.shape[3]
    depth = pulses * size

    def at(offset, k):
        return lax.rem(chip + offset + chips, chips) * 2 + k

    def dev(i):
        return {"shard": i}

    partner = chip * 2 + 1 - core

    loads = {}

    def load(name, src, dst, i):
        loads[name] = pltpu.make_async_copy(src, dst, in_sem.at[i])
        loads[name].start()

    load("x0", echoes.at[0, :, 0], x_in.at[0], 0)
    load("ta", tab_a, ta, 1)
    load("tw", twid, tw, 2)
    load("tb", tab_b, tb, 3)
    load("w", waveform, w_in, 4)
    for b in range(1, beams):
        load(f"x{b}", echoes.at[0, :, b], x_in.at[b], 4 + b)

    barrier = pltpu.get_barrier_semaphore()
    peers = [(d, k) for d in range(-HOP, HOP + 1) for k in (0, 1) if d]
    for d, k in peers:
        pl.semaphore_signal(barrier, inc=1, device_id=dev(at(d, k)), device_id_type=MESH)
    pl.semaphore_signal(barrier, inc=1, device_id=dev(partner), device_id_type=MESH)

    def range_compress(b):
        loads[f"x{b}"].wait()
        for ri in range(2):
            for j in range(GA):
                x_rows[ri, j * pulses : (j + 1) * pulses, :] = x_in[b, ri, :, j * GB : (j + 1) * GB]
        if b == 0:
            loads["w"].wait()
            for ri in range(2):
                for j in range(GA):
                    grid[ri * GA + j : ri * GA + j + 1, :] = w_in[ri : ri + 1, j * GB : (j + 1) * GB]
            fr, fi = filter_grid(grid[...])
            filt[0] = fr
            filt[1] = fi
            for name in ("ta", "tw", "tb"):
                loads[name].wait()
        rows = [
            [x_rows[ri, pl.ds(p, GA, stride=pulses), :] for p in range(pulses)] for ri in range(2)
        ]
        done = compress(
            rows[0], rows[1], ta[0], ta[1], tb[0], tb[1], tw[0], tw[1], filt[0], filt[1]
        )
        scale = 1.0 / (GA * GB * math.sqrt(depth))
        for p in range(pulses):
            weight = taper[me * pulses + p] * scale
            for ri in range(2):
                own[b, ri, pl.ds(p, GA, stride=pulses), :] = (
                    done[ri * GA : (ri + 1) * GA, p * GB : (p + 1) * GB] * weight
                )
        mine = pl.ds(pl.multiple_of(me * pulses, pulses), pulses)
        recv[b, :, mine, :] = own[b, :, mine, :]

    def rows_of(i, n=1):
        return pl.ds(pl.multiple_of(i * pulses, pulses), n * pulses)

    def first_leg(b, side, e):
        step = 1 - 2 * side
        far = at(step * (HOP + e), 0)
        to = dev(at(step * HOP, core))
        if e == HOP:
            src = own.at[b, :, rows_of(far + side)]
            dst = land.at[b, side, e - 1, :, pl.ds(side * pulses, pulses)]
        else:
            src = own.at[b, :, rows_of(far, 2)]
            dst = land.at[b, side, e - 1]
        return pltpu.make_async_remote_copy(
            src_ref=src,
            dst_ref=dst,
            send_sem=own_sem.at[b],
            recv_sem=land_sem.at[b, side, e - 1],
            device_id=to,
            device_id_type=MESH,
        )

    def direct(b, to):
        return pltpu.make_async_remote_copy(
            src_ref=own.at[b, :, rows_of(to)],
            dst_ref=recv.at[b, :, rows_of(me)],
            send_sem=own_sem.at[b],
            recv_sem=recv_sem.at[b],
            device_id=dev(to),
            device_id_type=MESH,
        )

    def second_leg(b, side, e, k):
        step = 1 - 2 * side
        src = at(-step * HOP, core)
        return pltpu.make_async_remote_copy(
            src_ref=land.at[b, side, e - 1, :, pl.ds(k * pulses, pulses)],
            dst_ref=recv.at[b, :, rows_of(src)],
            send_sem=next_sem.at[b],
            recv_sem=recv_sem.at[b],
            device_id=dev(at(step * e, k)),
            device_id_type=MESH,
        )

    def start_first(b):
        for e in range(HOP, 0, -1):
            for side in range(2):
                first_leg(b, side, e).start()

    def start_near(b):
        for e in range(HOP, 0, -1):
            for k in range(2):
                for side in range(2):
                    direct(b, at((1 - 2 * side) * e, k)).start()
        direct(b, partner).start()

    def start_second(b):
        for e in range(HOP, 0, -1):
            for side in range(2):
                first_leg(b, side, e).wait_recv()
                for k in (side,) if e == HOP else (0, 1):
                    second_leg(b, side, e, k).start()

    def wait_blocks(sem, n):
        ref = own.at[0, :, pl.ds(0, n * pulses)]
        pltpu.make_async_copy(ref, ref, sem).wait()

    def halo_copy(b, side):
        to = lax.rem(me + (1 if side else size - 1), size)
        return pltpu.make_async_remote_copy(
            src_ref=halo_out.at[b, side],
            dst_ref=halo_in.at[b, 1 - side],
            send_sem=hs_sem.at[b, side],
            recv_sem=hr_sem.at[b, 1 - side],
            device_id=dev(to),
            device_id_type=MESH,
        )

    def doppler(b):
        rows = [
            [recv[b, ri, pl.ds(l, size, stride=pulses), :] for l in range(pulses)] for ri in range(2)
        ]
        value = doppler_power(
            rows[0], rows[1], ta[0], lambda l: (dop[0, :, l * GB : (l + 1) * GB], dop[1, :, l * GB : (l + 1) * GB])
        )
        halo_out[b, 0] = pack(value, 0)
        halo_out[b, 1] = pack(value, GB - HALO)
        power[b] = value
        for side in range(2):
            halo_copy(b, side).start()

    def cfar(b):
        own_band, left_band, right_band = bands(guard[b], train[b])
        cells = power[b]
        high, low = split(cells)
        band = own_band.astype(BF16)
        total = jnp.dot(
            jnp.concatenate([high, low], axis=1),
            jnp.concatenate([band, band], axis=0),
            preferred_element_type=F32,
        )
        slot = lax.div(lax.broadcasted_iota(jnp.int32, (GB, GB), 0), 32)
        rows = depth // 4
        for side in range(2):
            halo_copy(b, side).wait_send()
            halo_copy(b, 1 - side).wait_recv()
        left = jnp.where(me > 0, halo_in[b, 0], 0.0)
        right = jnp.where(me < size - 1, halo_in[b, 1], 0.0)
        lh, ll = split(left)
        rh, rl = split(right)
        edges = jnp.concatenate([lh, ll, rh, rl], axis=1)
        floor = noise[b]
        inverse = 1.0 / (2.0 * train[b].astype(F32))
        for r in range(4):
            here = slot == r
            lb = jnp.where(here, left_band, 0.0).astype(BF16)
            rb = jnp.where(here, right_band, 0.0).astype(BF16)
            more = jnp.dot(
                edges, jnp.concatenate([lb, lb, rb, rb], axis=0), preferred_element_type=F32
            )
            window = total[r * rows : (r + 1) * rows] + more
            result[b, r * rows : (r + 1) * rows, :] = cells[r * rows : (r + 1) * rows] / (
                floor + window * inverse
            )
        pltpu.make_async_copy(result.at[b], out.at[0, b], out_sem.at[b]).start()

    range_compress(0)
    pl.semaphore_wait(barrier, len(peers) + 1)
    start_first(0)
    start_near(0)
    for b in range(1, beams):
        range_compress(b)
    for l in range(pulses):
        for i in range(2):
            col = i * pulses + l
            dop[i, :, l * GB : (l + 1) * GB] = jnp.broadcast_to(tw[2, :, col : col + 1], (GA, GB))
    for b in range(beams):
        start_second(b)
        if b + 1 < beams:
            start_first(b + 1)
            start_near(b + 1)
        if b > 0:
            cfar(b - 1)
        wait_blocks(recv_sem.at[b], size - 1)
        doppler(b)
    cfar(beams - 1)
    for b in range(beams):
        wait_blocks(own_sem.at[b], size - 1)
        wait_blocks(next_sem.at[b], 4 * HOP - 2)
        pltpu.make_async_copy(result.at[b], out.at[0, b], out_sem.at[b]).wait()


def solution(mesh):
    size = mesh.shape["shard"]

    def step(echoes, waveform, taper, guard, train, noise):
        _, _, beams, pulses, gates = echoes.shape
        depth = pulses * size
        tab_a, tab_b, twid = tables(depth)
        hbm = pl.BlockSpec(memory_space=pl.ANY)
        smem = pl.BlockSpec(memory_space=pltpu.SMEM)
        vmem = pltpu.VMEM
        dma = pltpu.SemaphoreType.DMA
        return pl.pallas_call(
            functools.partial(kernel, size),
            out_shape=jax.ShapeDtypeStruct((1, beams, depth, GB), F32),
            in_specs=[hbm, hbm, smem, smem, smem, smem, hbm, hbm, hbm],
            out_specs=hbm,
            scratch_shapes=[
                vmem((beams, 2, pulses, gates), F32),
                vmem((2, gates), F32),
                vmem(tab_a.shape, BF16),
                vmem(tab_b.shape, BF16),
                vmem(twid.shape, F32),
                vmem((2, GA * pulses, GB), F32),
                vmem((GB, GB), F32),
                vmem((2, GA, GB), F32),
                vmem((beams, 2, depth, GB), F32),
                vmem((beams, 2, depth, GB), F32),
                vmem((beams, 2, HOP, 2, 2 * pulses, GB), F32),
                vmem((2, GA, pulses * GB), F32),
                vmem((beams, depth, GB), F32),
                vmem((beams, 2, depth // 4, GB), F32),
                vmem((beams, 2, depth // 4, GB), F32),
                vmem((beams, depth, GB), F32),
                dma((4 + beams,)),
                dma((beams,)),
                dma((beams,)),
                dma((beams,)),
                dma((beams, 2, HOP)),
                dma((beams, 2)),
                dma((beams, 2)),
                dma((beams,)),
            ],
            compiler_params=pltpu.CompilerParams(
                collective_id=0, has_side_effects=True, vmem_limit_bytes=56 * 2**20
            ),
            name="pulse_doppler",
        )(echoes, waveform, taper, guard, train, noise, jnp.asarray(tab_a), jnp.asarray(tab_b), jnp.asarray(twid))

    in_specs = (
        P(None, None, "groups", "shard", None),
        P(),
        P(),
        P("groups"),
        P("groups"),
        P("groups"),
    )
    out_specs = P(None, "groups", None, "shard")
    return jax.shard_map(step, mesh=mesh, in_specs=in_specs, out_specs=out_specs, check_vma=False)
```

```python
import functools
import math

import jax
import jax.numpy as jnp
import numpy as np
from jax import lax
from jax.experimental import pallas as pl
from jax.experimental.pallas import tpu as pltpu
from jax.sharding import PartitionSpec as P

MESH = pl.DeviceIdType.MESH
GA = 64
GB = 128
HALO = 20
HOP = 8
F32 = jnp.float32
BF16 = jnp.bfloat16


def split_host(table):
    high = table.astype(np.float32).astype(jnp.bfloat16)
    low = (table - high.astype(np.float64)).astype(np.float32).astype(jnp.bfloat16)
    return high, low


def tables(pulses):
    a = np.arange(GA)
    n = np.arange(GB)
    c = np.concatenate([np.arange(0, GB, 2), np.arange(1, GB, 2)])
    ang_a = 2 * math.pi / GA * (np.outer(a, a) % GA)
    ang_b = 2 * math.pi / GB * (np.outer(n, c) % GB)
    ca, sa = np.cos(ang_a), np.sin(ang_a)
    cb, sb = np.cos(ang_b), np.sin(ang_b)
    fwd_a = np.block([[ca, sa], [-sa, ca]])
    inv_a = np.block([[ca, -sa], [sa, ca]])
    fwd_b = np.block([[cb, -sb], [sb, cb]])
    inv_b = np.block([[cb.T, sb.T], [-sb.T, cb.T]])

    def left(m):
        h, l = split_host(m)
        return np.concatenate([h, h, l], axis=1)

    def right(m):
        h, l = split_host(m)
        return np.concatenate([h, h, l], axis=0)

    ang_t = 2 * math.pi / (GA * GB) * (np.outer(a, n) % (GA * GB))
    radix = pulses // GA
    ang_d = 2 * math.pi / pulses * (np.outer(a, np.arange(radix)) % pulses)
    small = np.zeros((GA, GB))
    small[:, :radix] = np.cos(ang_d)
    small[:, radix : 2 * radix] = np.sin(ang_d)
    twid = np.stack([np.cos(ang_t), np.sin(ang_t), small]).astype(np.float32)
    return (
        np.stack([left(fwd_a), left(inv_a)]),
        np.stack([right(fwd_b), right(inv_b)]),
        twid,
    )


def split(x):
    high = x.astype(BF16)
    return high, (x - high.astype(F32)).astype(BF16)


def dot_left(table, values):
    high, low = split(values)
    return jnp.dot(table, jnp.concatenate([high, low, high], axis=0), preferred_element_type=F32)


def dot_right(values, table):
    high, low = split(values)
    return jnp.dot(jnp.concatenate([high, low, high], axis=1), table, preferred_element_type=F32)


def compress(rows_re, rows_im, fwd_a, inv_a, fwd_b, inv_b, tc, ts, fr, fi):
    count = len(rows_re)
    x = jnp.concatenate(
        [jnp.concatenate(rows_re, axis=1), jnp.concatenate(rows_im, axis=1)], axis=0
    )
    y = dot_left(fwd_a, x)
    parts = []
    for p in range(count):
        yr = y[:GA, p * GB : (p + 1) * GB]
        yi = y[GA:, p * GB : (p + 1) * GB]
        parts.append(jnp.concatenate([yr * tc + yi * ts, yi * tc - yr * ts], axis=1))
    z = dot_right(jnp.concatenate(parts, axis=0), fwd_b)
    parts = []
    for p in range(count):
        zr = z[p * GA : (p + 1) * GA, :GB]
        zi = z[p * GA : (p + 1) * GA, GB:]
        parts.append(jnp.concatenate([zr * fr + zi * fi, zi * fr - zr * fi], axis=1))
    v = dot_right(jnp.concatenate(parts, axis=0), inv_b)
    re, im = [], []
    for p in range(count):
        vr = v[p * GA : (p + 1) * GA, :GB]
        vi = v[p * GA : (p + 1) * GA, GB:]
        re.append(vr * tc - vi * ts)
        im.append(vr * ts + vi * tc)
    return dot_left(
        inv_a,
        jnp.concatenate([jnp.concatenate(re, axis=1), jnp.concatenate(im, axis=1)], axis=0),
    )


def butterfly8(xs):
    r = math.sqrt(0.5)

    def add(u, v):
        return u[0] + v[0], u[1] + v[1]

    def sub(u, v):
        return u[0] - v[0], u[1] - v[1]

    def dft4(q):
        s02, d02 = add(q[0], q[2]), sub(q[0], q[2])
        s13, d13 = add(q[1], q[3]), sub(q[1], q[3])
        turned = (d13[1], -d13[0])
        return [add(s02, s13), add(d02, turned), sub(s02, s13), sub(d02, turned)]

    even, odd = dft4(xs[0::2]), dft4(xs[1::2])
    o1 = ((odd[1][0] + odd[1][1]) * r, (odd[1][1] - odd[1][0]) * r)
    o2 = (odd[2][1], -odd[2][0])
    o3 = ((odd[3][1] - odd[3][0]) * r, -(odd[3][0] + odd[3][1]) * r)
    odd = [odd[0], o1, o2, o3]
    return [add(even[k], odd[k]) for k in range(4)] + [sub(even[k], odd[k]) for k in range(4)]


def doppler_power(rows_re, rows_im, fwd_a, turn):
    count = len(rows_re)
    x = jnp.concatenate(
        [jnp.concatenate(rows_re, axis=1), jnp.concatenate(rows_im, axis=1)], axis=0
    )
    y = dot_left(fwd_a, x)
    terms = []
    for l in range(count):
        yr = y[:GA, l * GB : (l + 1) * GB]
        yi = y[GA:, l * GB : (l + 1) * GB]
        if l == 0:
            terms.append((yr, yi))
        else:
            dc, ds = turn(l)
            terms.append((yr * dc + yi * ds, yi * dc - yr * ds))
    return jnp.concatenate([r * r + i * i for r, i in butterfly8(terms)], axis=0)


def filter_grid(grid):
    turned = grid.T
    top, bottom = turned[:GA], turned[GA:]
    low = lax.broadcasted_iota(jnp.int32, (GA, GB), 1) < GA
    fr = jnp.where(low, top, pltpu.roll(bottom, GA, 1))
    fi = jnp.where(low, pltpu.roll(top, GA, 1), bottom)
    return fr, fi


def bands(guard, train):
    i = lax.broadcasted_iota(jnp.int32, (GB, GB), 0)
    j = lax.broadcasted_iota(jnp.int32, (GB, GB), 1)

    def inside(d):
        return jnp.where((d > guard) & (d <= guard + train), 1.0, 0.0).astype(F32)

    own = inside(jnp.abs(i - j))
    slot = lax.rem(i, 32)
    used = jnp.where(slot < HALO, 1.0, 0.0).astype(F32)
    left = inside(j + HALO - slot) * used
    right = inside(slot + GB - j) * used
    return own, left, right


def pack(power, lo):
    rows = power.shape[0] // 4
    lane = lax.broadcasted_iota(jnp.int32, (rows, GB), 1)
    out = None
    for r in range(4):
        block = power[r * rows : (r + 1) * rows]
        shift = (32 * r - lo) % GB
        moved = pltpu.roll(block, shift, 1) if shift else block
        out = moved if out is None else jnp.where(lane >= 32 * r, moved, out)
    return out


def kernel(
    size,
    echoes,
    waveform,
    taper,
    guard,
    train,
    noise,
    tab_a,
    tab_b,
    twid,
    out,
    x_in,
    w_in,
    ta,
    tb,
    tw,
    x_rows,
    grid,
    filt,
    own,
    recv,
    dop,
    power,
    halo_out,
    halo_in,
    result,
    in_sem,
    own_sem,
    recv_sem,
    ready,
    hs_sem,
    hr_sem,
    out_sem,
):
    chips = size // 2
    me = lax.axis_index("shard")
    chip = lax.div(me, 2)
    core = lax.rem(me, 2)
    beams = echoes.shape[2]
    pulses = echoes.shape[3]
    depth = pulses * size

    def at(offset, k):
        return lax.rem(chip + offset + chips, chips) * 2 + k

    def dev(i):
        return {"shard": i}

    partner = chip * 2 + 1 - core

    loads = {}

    def load(name, src, dst, i):
        loads[name] = pltpu.make_async_copy(src, dst, in_sem.at[i])
        loads[name].start()

    load("x0", echoes.at[0, :, 0], x_in.at[0], 0)
    load("ta", tab_a, ta, 1)
    load("tw", twid, tw, 2)
    load("tb", tab_b, tb, 3)
    load("w", waveform, w_in, 4)
    for b in range(1, beams):
        load(f"x{b}", echoes.at[0, :, b], x_in.at[b], 4 + b)

    barrier = pltpu.get_barrier_semaphore()
    peers = [(d, k) for d in range(-HOP, HOP + 1) for k in (0, 1) if d]
    for d, k in peers:
        pl.semaphore_signal(barrier, inc=1, device_id=dev(at(d, k)), device_id_type=MESH)
    pl.semaphore_signal(barrier, inc=1, device_id=dev(partner), device_id_type=MESH)

    def range_compress(b):
        loads[f"x{b}"].wait()
        for ri in range(2):
            for j in range(GA):
                x_rows[ri, j * pulses : (j + 1) * pulses, :] = x_in[b, ri, :, j * GB : (j + 1) * GB]
        if b == 0:
            loads["w"].wait()
            for ri in range(2):
                for j in range(GA):
                    grid[ri * GA + j : ri * GA + j + 1, :] = w_in[ri : ri + 1, j * GB : (j + 1) * GB]
            fr, fi = filter_grid(grid[...])
            filt[0] = fr
            filt[1] = fi
            for name in ("ta", "tw", "tb"):
                loads[name].wait()
        rows = [
            [x_rows[ri, pl.ds(p, GA, stride=pulses), :] for p in range(pulses)] for ri in range(2)
        ]
        done = compress(
            rows[0], rows[1], ta[0], ta[1], tb[0], tb[1], tw[0], tw[1], filt[0], filt[1]
        )
        scale = 1.0 / (GA * GB * math.sqrt(depth))
        for p in range(pulses):
            weight = taper[me * pulses + p] * scale
            for ri in range(2):
                own[b, ri, pl.ds(p, GA, stride=pulses), :] = (
                    done[ri * GA : (ri + 1) * GA, p * GB : (p + 1) * GB] * weight
                )
        mine = pl.ds(pl.multiple_of(me * pulses, pulses), pulses)
        recv[b, :, mine, :] = own[b, :, mine, :]

    def rows_of(i, n=1):
        return pl.ds(pl.multiple_of(i * pulses, pulses), n * pulses)

    def direct(b, to):
        return pltpu.make_async_remote_copy(
            src_ref=own.at[b, :, rows_of(to)],
            dst_ref=recv.at[b, :, rows_of(me)],
            send_sem=own_sem.at[b],
            recv_sem=recv_sem.at[b],
            device_id=dev(to),
            device_id_type=MESH,
        )

    def start_near(b):
        direct(b, partner).start()
        for e in range(1, HOP + 1):
            for k in range(2):
                for step in (1, -1):
                    direct(b, at(step * e, k)).start()

    def start_far(b):
        for e in range(HOP + 1, chips // 2):
            for k in range(2):
                for step in (1, -1):
                    direct(b, at(step * e, k)).start()
        for k in range(2):
            direct(b, at(chips // 2, k)).start()

    def start_by_place(b):
        half = chips // 2
        late = chip >= half

        def opposite():
            for k in range(2):
                direct(b, at(half, k)).start()

        direct(b, partner).start()
        pl.when(late)(opposite)
        up = jnp.where(late, chips - chip, 1)
        down = jnp.minimum(chip, half - 1)
        for i in range(half - 1):
            forward = lax.rem(up - 1 + i, half - 1) + 1
            backward = lax.rem(down - 1 - i + 2 * (half - 1), half - 1) + 1
            for k in range(2):
                direct(b, at(forward, k)).start()
                direct(b, at(-backward, k)).start()
        pl.when(jnp.logical_not(late))(opposite)

    def wait_blocks(sem, n):
        ref = own.at[0, :, pl.ds(0, n * pulses)]
        pltpu.make_async_copy(ref, ref, sem).wait()

    def halo_copy(b, side):
        to = lax.rem(me + (1 if side else size - 1), size)
        return pltpu.make_async_remote_copy(
            src_ref=halo_out.at[b, side],
            dst_ref=halo_in.at[b, 1 - side],
            send_sem=hs_sem.at[b, side],
            recv_sem=hr_sem.at[b, 1 - side],
            device_id=dev(to),
            device_id_type=MESH,
        )

    def doppler(b):
        rows = [
            [recv[b, ri, pl.ds(l, size, stride=pulses), :] for l in range(pulses)] for ri in range(2)
        ]
        value = doppler_power(
            rows[0], rows[1], ta[0], lambda l: (dop[0, :, l * GB : (l + 1) * GB], dop[1, :, l * GB : (l + 1) * GB])
        )
        halo_out[b, 0] = pack(value, 0)
        halo_out[b, 1] = pack(value, GB - HALO)
        power[b] = value
        for side in range(2):
            halo_copy(b, side).start()

    def cfar(b):
        own_band, left_band, right_band = bands(guard[b], train[b])
        cells = power[b]
        high, low = split(cells)
        band = own_band.astype(BF16)
        total = jnp.dot(
            jnp.concatenate([high, low], axis=1),
            jnp.concatenate([band, band], axis=0),
            preferred_element_type=F32,
        )
        slot = lax.div(lax.broadcasted_iota(jnp.int32, (GB, GB), 0), 32)
        rows = depth // 4
        for side in range(2):
            halo_copy(b, side).wait_send()
            halo_copy(b, 1 - side).wait_recv()
        left = jnp.where(me > 0, halo_in[b, 0], 0.0)
        right = jnp.where(me < size - 1, halo_in[b, 1], 0.0)
        lh, ll = split(left)
        rh, rl = split(right)
        edges = jnp.concatenate([lh, ll, rh, rl], axis=1)
        floor = noise[b]
        inverse = 1.0 / (2.0 * train[b].astype(F32))
        for r in range(4):
            here = slot == r
            lb = jnp.where(here, left_band, 0.0).astype(BF16)
            rb = jnp.where(here, right_band, 0.0).astype(BF16)
            more = jnp.dot(
                edges, jnp.concatenate([lb, lb, rb, rb], axis=0), preferred_element_type=F32
            )
            window = total[r * rows : (r + 1) * rows] + more
            result[b, r * rows : (r + 1) * rows, :] = cells[r * rows : (r + 1) * rows] / (
                floor + window * inverse
            )
        pltpu.make_async_copy(result.at[b], out.at[0, b], out_sem.at[b]).start()

    range_compress(0)
    pl.semaphore_wait(barrier, len(peers) + 1)
    for step in (1, -1):
        pl.semaphore_signal(ready, inc=1, device_id=dev(at(step * HOP, core)), device_id_type=MESH)
    start_near(0)
    for b in range(1, beams):
        range_compress(b)
    pl.semaphore_wait(ready, 2)
    start_far(0)
    for b in range(1, beams):
        start_by_place(b)
    for l in range(pulses):
        for i in range(2):
            col = i * pulses + l
            dop[i, :, l * GB : (l + 1) * GB] = jnp.broadcast_to(tw[2, :, col : col + 1], (GA, GB))
    for b in range(beams):
        wait_blocks(recv_sem.at[b], size - 1)
        doppler(b)
        cfar(b)
    for b in range(beams):
        wait_blocks(own_sem.at[b], size - 1)
        pltpu.make_async_copy(result.at[b], out.at[0, b], out_sem.at[b]).wait()


def solution(mesh):
    size = mesh.shape["shard"]

    def step(echoes, waveform, taper, guard, train, noise):
        _, _, beams, pulses, gates = echoes.shape
        depth = pulses * size
        tab_a, tab_b, twid = tables(depth)
        hbm = pl.BlockSpec(memory_space=pl.ANY)
        smem = pl.BlockSpec(memory_space=pltpu.SMEM)
        vmem = pltpu.VMEM
        dma = pltpu.SemaphoreType.DMA
        return pl.pallas_call(
            functools.partial(kernel, size),
            out_shape=jax.ShapeDtypeStruct((1, beams, depth, GB), F32),
            in_specs=[hbm, hbm, smem, smem, smem, smem, hbm, hbm, hbm],
            out_specs=hbm,
            scratch_shapes=[
                vmem((beams, 2, pulses, gates), F32),
                vmem((2, gates), F32),
                vmem(tab_a.shape, BF16),
                vmem(tab_b.shape, BF16),
                vmem(twid.shape, F32),
                vmem((2, GA * pulses, GB), F32),
                vmem((GB, GB), F32),
                vmem((2, GA, GB), F32),
                vmem((beams, 2, depth, GB), F32),
                vmem((beams, 2, depth, GB), F32),
                vmem((2, GA, pulses * GB), F32),
                vmem((beams, depth, GB), F32),
                vmem((beams, 2, depth // 4, GB), F32),
                vmem((beams, 2, depth // 4, GB), F32),
                vmem((beams, depth, GB), F32),
                dma((4 + beams,)),
                dma((beams,)),
                dma((beams,)),
                pltpu.SemaphoreType.REGULAR,
                dma((beams, 2)),
                dma((beams, 2)),
                dma((beams,)),
            ],
            compiler_params=pltpu.CompilerParams(
                collective_id=0, has_side_effects=True, vmem_limit_bytes=56 * 2**20
            ),
            name="pulse_doppler",
        )(echoes, waveform, taper, guard, train, noise, jnp.asarray(tab_a), jnp.asarray(tab_b), jnp.asarray(twid))

    in_specs = (
        P(None, None, "groups", "shard", None),
        P(),
        P(),
        P("groups"),
        P("groups"),
        P("groups"),
    )
    out_specs = P(None, "groups", None, "shard")
    return jax.shard_map(step, mesh=mesh, in_specs=in_specs, out_specs=out_specs, check_vma=False)
```

```python
import functools
import math

import jax
import jax.numpy as jnp
import numpy as np
from jax import lax
from jax.experimental import pallas as pl
from jax.experimental.pallas import tpu as pltpu
from jax.sharding import PartitionSpec as P

MESH = pl.DeviceIdType.MESH
GA = 64
GB = 128
HALO = 20
HOP = 8
F32 = jnp.float32
BF16 = jnp.bfloat16


def split_host(table):
    high = table.astype(np.float32).astype(jnp.bfloat16)
    low = (table - high.astype(np.float64)).astype(np.float32).astype(jnp.bfloat16)
    return high, low


def tables(pulses):
    a = np.arange(GA)
    n = np.arange(GB)
    c = np.concatenate([np.arange(0, GB, 2), np.arange(1, GB, 2)])
    ang_a = 2 * math.pi / GA * (np.outer(a, a) % GA)
    ang_b = 2 * math.pi / GB * (np.outer(n, c) % GB)
    ca, sa = np.cos(ang_a), np.sin(ang_a)
    cb, sb = np.cos(ang_b), np.sin(ang_b)
    fwd_a = np.block([[ca, sa], [-sa, ca]])
    inv_a = np.block([[ca, -sa], [sa, ca]])
    fwd_b = np.block([[cb, -sb], [sb, cb]])
    inv_b = np.block([[cb.T, sb.T], [-sb.T, cb.T]])

    def left(m):
        h, l = split_host(m)
        return np.concatenate([h, h, l], axis=1)

    def right(m):
        h, l = split_host(m)
        return np.concatenate([h, h, l], axis=0)

    ang_t = 2 * math.pi / (GA * GB) * (np.outer(a, n) % (GA * GB))
    radix = pulses // GA
    ang_d = 2 * math.pi / pulses * (np.outer(a, np.arange(radix)) % pulses)
    small = np.zeros((GA, GB))
    small[:, :radix] = np.cos(ang_d)
    small[:, radix : 2 * radix] = np.sin(ang_d)
    twid = np.stack([np.cos(ang_t), np.sin(ang_t), small]).astype(np.float32)
    return (
        np.stack([left(fwd_a), left(inv_a)]),
        np.stack([right(fwd_b), right(inv_b)]),
        twid,
    )


def split(x):
    high = x.astype(BF16)
    return high, (x - high.astype(F32)).astype(BF16)


def dot_left(table, values):
    high, low = split(values)
    return jnp.dot(table, jnp.concatenate([high, low, high], axis=0), preferred_element_type=F32)


def dot_right(values, table):
    high, low = split(values)
    return jnp.dot(jnp.concatenate([high, low, high], axis=1), table, preferred_element_type=F32)


def compress(rows_re, rows_im, fwd_a, inv_a, fwd_b, inv_b, tc, ts, fr, fi):
    count = len(rows_re)
    x = jnp.concatenate(
        [jnp.concatenate(rows_re, axis=1), jnp.concatenate(rows_im, axis=1)], axis=0
    )
    y = dot_left(fwd_a, x)
    parts = []
    for p in range(count):
        yr = y[:GA, p * GB : (p + 1) * GB]
        yi = y[GA:, p * GB : (p + 1) * GB]
        parts.append(jnp.concatenate([yr * tc + yi * ts, yi * tc - yr * ts], axis=1))
    z = dot_right(jnp.concatenate(parts, axis=0), fwd_b)
    parts = []
    for p in range(count):
        zr = z[p * GA : (p + 1) * GA, :GB]
        zi = z[p * GA : (p + 1) * GA, GB:]
        parts.append(jnp.concatenate([zr * fr + zi * fi, zi * fr - zr * fi], axis=1))
    v = dot_right(jnp.concatenate(parts, axis=0), inv_b)
    re, im = [], []
    for p in range(count):
        vr = v[p * GA : (p + 1) * GA, :GB]
        vi = v[p * GA : (p + 1) * GA, GB:]
        re.append(vr * tc - vi * ts)
        im.append(vr * ts + vi * tc)
    return dot_left(
        inv_a,
        jnp.concatenate([jnp.concatenate(re, axis=1), jnp.concatenate(im, axis=1)], axis=0),
    )


def butterfly8(xs):
    r = math.sqrt(0.5)

    def add(u, v):
        return u[0] + v[0], u[1] + v[1]

    def sub(u, v):
        return u[0] - v[0], u[1] - v[1]

    def dft4(q):
        s02, d02 = add(q[0], q[2]), sub(q[0], q[2])
        s13, d13 = add(q[1], q[3]), sub(q[1], q[3])
        turned = (d13[1], -d13[0])
        return [add(s02, s13), add(d02, turned), sub(s02, s13), sub(d02, turned)]

    even, odd = dft4(xs[0::2]), dft4(xs[1::2])
    o1 = ((odd[1][0] + odd[1][1]) * r, (odd[1][1] - odd[1][0]) * r)
    o2 = (odd[2][1], -odd[2][0])
    o3 = ((odd[3][1] - odd[3][0]) * r, -(odd[3][0] + odd[3][1]) * r)
    odd = [odd[0], o1, o2, o3]
    return [add(even[k], odd[k]) for k in range(4)] + [sub(even[k], odd[k]) for k in range(4)]


def doppler_power(rows_re, rows_im, fwd_a, turn):
    count = len(rows_re)
    x = jnp.concatenate(
        [jnp.concatenate(rows_re, axis=1), jnp.concatenate(rows_im, axis=1)], axis=0
    )
    y = dot_left(fwd_a, x)
    terms = []
    for l in range(count):
        yr = y[:GA, l * GB : (l + 1) * GB]
        yi = y[GA:, l * GB : (l + 1) * GB]
        if l == 0:
            terms.append((yr, yi))
        else:
            dc, ds = turn(l)
            terms.append((yr * dc + yi * ds, yi * dc - yr * ds))
    return jnp.concatenate([r * r + i * i for r, i in butterfly8(terms)], axis=0)


def filter_grid(grid):
    turned = grid.T
    top, bottom = turned[:GA], turned[GA:]
    low = lax.broadcasted_iota(jnp.int32, (GA, GB), 1) < GA
    fr = jnp.where(low, top, pltpu.roll(bottom, GA, 1))
    fi = jnp.where(low, pltpu.roll(top, GA, 1), bottom)
    return fr, fi


def bands(guard, train):
    i = lax.broadcasted_iota(jnp.int32, (GB, GB), 0)
    j = lax.broadcasted_iota(jnp.int32, (GB, GB), 1)

    def inside(d):
        return jnp.where((d > guard) & (d <= guard + train), 1.0, 0.0).astype(F32)

    own = inside(jnp.abs(i - j))
    slot = lax.rem(i, 32)
    used = jnp.where(slot < HALO, 1.0, 0.0).astype(F32)
    left = inside(j + HALO - slot) * used
    right = inside(slot + GB - j) * used
    return own, left, right


def pack(power, lo):
    rows = power.shape[0] // 4
    lane = lax.broadcasted_iota(jnp.int32, (rows, GB), 1)
    out = None
    for r in range(4):
        block = power[r * rows : (r + 1) * rows]
        shift = (32 * r - lo) % GB
        moved = pltpu.roll(block, shift, 1) if shift else block
        out = moved if out is None else jnp.where(lane >= 32 * r, moved, out)
    return out


def kernel(
    size,
    echoes,
    waveform,
    taper,
    guard,
    train,
    noise,
    tab_a,
    tab_b,
    twid,
    out,
    x_in,
    w_in,
    ta,
    tb,
    tw,
    x_rows,
    grid,
    filt,
    own,
    recv,
    dop,
    power,
    halo_out,
    halo_in,
    in_sem,
    own_sem,
    recv_sem,
    ready,
    hs_sem,
    hr_sem,
):
    chips = size // 2
    me = lax.axis_index("shard")
    chip = lax.div(me, 2)
    core = lax.rem(me, 2)
    beams = echoes.shape[2]
    pulses = echoes.shape[3]
    depth = pulses * size

    def at(offset, k):
        return lax.rem(chip + offset + chips, chips) * 2 + k

    def dev(i):
        return {"shard": i}

    partner = chip * 2 + 1 - core

    loads = {}

    def load(name, src, dst, i):
        loads[name] = pltpu.make_async_copy(src, dst, in_sem.at[i])
        loads[name].start()

    load("x0", echoes.at[0, :, 0], x_in.at[0], 0)
    load("ta", tab_a, ta, 1)
    load("tw", twid, tw, 2)
    load("tb", tab_b, tb, 3)
    load("w", waveform, w_in, 4)
    for b in range(1, beams):
        load(f"x{b}", echoes.at[0, :, b], x_in.at[b], 4 + b)

    barrier = pltpu.get_barrier_semaphore()
    peers = [(d, k) for d in range(-HOP, HOP + 1) for k in (0, 1) if d]
    for d, k in peers:
        pl.semaphore_signal(barrier, inc=1, device_id=dev(at(d, k)), device_id_type=MESH)
    pl.semaphore_signal(barrier, inc=1, device_id=dev(partner), device_id_type=MESH)

    def range_compress(b):
        loads[f"x{b}"].wait()
        for ri in range(2):
            for j in range(GA):
                x_rows[ri, j * pulses : (j + 1) * pulses, :] = x_in[b, ri, :, j * GB : (j + 1) * GB]
        if b == 0:
            loads["w"].wait()
            for ri in range(2):
                for j in range(GA):
                    grid[ri * GA + j : ri * GA + j + 1, :] = w_in[ri : ri + 1, j * GB : (j + 1) * GB]
            fr, fi = filter_grid(grid[...])
            filt[0] = fr
            filt[1] = fi
            for name in ("ta", "tw", "tb"):
                loads[name].wait()
        rows = [
            [x_rows[ri, pl.ds(p, GA, stride=pulses), :] for p in range(pulses)] for ri in range(2)
        ]
        done = compress(
            rows[0], rows[1], ta[0], ta[1], tb[0], tb[1], tw[0], tw[1], filt[0], filt[1]
        )
        scale = 1.0 / (GA * GB * math.sqrt(depth))
        for p in range(pulses):
            weight = taper[me * pulses + p] * scale
            for ri in range(2):
                own[b, ri, pl.ds(p, GA, stride=pulses), :] = (
                    done[ri * GA : (ri + 1) * GA, p * GB : (p + 1) * GB] * weight
                )
        mine = pl.ds(pl.multiple_of(me * pulses, pulses), pulses)
        recv[b, :, mine, :] = own[b, :, mine, :]

    def rows_of(i, n=1):
        return pl.ds(pl.multiple_of(i * pulses, pulses), n * pulses)

    def direct(b, to):
        return pltpu.make_async_remote_copy(
            src_ref=own.at[b, :, rows_of(to)],
            dst_ref=recv.at[b, :, rows_of(me)],
            send_sem=own_sem.at[b],
            recv_sem=recv_sem.at[b],
            device_id=dev(to),
            device_id_type=MESH,
        )

    def start_by_place(b, lo, hi):
        half = chips // 2

        def both(offset):
            for k in range(2):
                direct(b, at(offset, k)).start()

        def when(condition, offset):
            pl.when(condition)(lambda: both(offset))

        def early():
            for m in range(1, half):
                if lo <= m <= hi:
                    both(m)
                if lo <= half - m <= hi:
                    when(half - m <= chip, m - half)
            for m in range(half - 1, 0, -1):
                if lo <= m <= hi:
                    when(m > chip, -m)
            if hi >= half:
                both(half)

        def late():
            if hi >= half:
                both(half)
            for place in range(half):
                up = chips - chip + place
                when((up >= lo) & (up <= min(hi, half - 1)), up)
                down = chip - place
                when((down >= lo) & (down <= min(hi, half - 1)), -down)
            for m in range(half - 1, 0, -1):
                if lo <= m <= hi:
                    when(chip + m < chips, m)
                    when(chip - m >= half, -m)

        if lo == 1:
            direct(b, partner).start()
        pl.when(chip < half)(early)
        pl.when(chip >= half)(late)

    def wait_blocks(sem, n):
        ref = own.at[0, :, pl.ds(0, n * pulses)]
        pltpu.make_async_copy(ref, ref, sem).wait()

    inner = (me > 0, me < size - 1)

    def halo_copy(b, side):
        to = lax.rem(me + (1 if side else size - 1), size)
        return pltpu.make_async_remote_copy(
            src_ref=halo_out.at[b, side],
            dst_ref=halo_in.at[b, 1 - side],
            send_sem=hs_sem.at[b, side],
            recv_sem=hr_sem.at[b, 1 - side],
            device_id=dev(to),
            device_id_type=MESH,
        )

    def doppler(b):
        rows = [
            [recv[b, ri, pl.ds(l, size, stride=pulses), :] for l in range(pulses)] for ri in range(2)
        ]
        value = doppler_power(
            rows[0], rows[1], ta[0], lambda l: (dop[0, :, l * GB : (l + 1) * GB], dop[1, :, l * GB : (l + 1) * GB])
        )
        halo_out[b, 0] = pack(value, 0)
        halo_out[b, 1] = pack(value, GB - HALO)
        power[b] = value
        for side in range(2):
            pl.when(inner[side])(halo_copy(b, side).start)

    def cfar(b):
        own_band, left_band, right_band = bands(guard[b], train[b])
        cells = power[b]
        high, low = split(cells)
        band = own_band.astype(BF16)
        total = jnp.dot(
            jnp.concatenate([high, low], axis=1),
            jnp.concatenate([band, band], axis=0),
            preferred_element_type=F32,
        )
        slot = lax.div(lax.broadcasted_iota(jnp.int32, (GB, GB), 0), 32)
        rows = depth // 4
        for side in range(2):

            def arrived():
                halo_copy(b, side).wait_send()
                halo_copy(b, 1 - side).wait_recv()

            def outside():
                halo_in[b, side] = jnp.zeros_like(halo_in[b, side])

            pl.when(inner[side])(arrived)
            pl.when(jnp.logical_not(inner[side]))(outside)
        left, right = halo_in[b, 0], halo_in[b, 1]
        lh, ll = split(left)
        rh, rl = split(right)
        edges = jnp.concatenate([lh, ll, rh, rl], axis=1)
        floor = noise[b]
        inverse = 1.0 / (2.0 * train[b].astype(F32))
        for r in range(4):
            here = slot == r
            lb = jnp.where(here, left_band, 0.0).astype(BF16)
            rb = jnp.where(here, right_band, 0.0).astype(BF16)
            more = jnp.dot(
                edges, jnp.concatenate([lb, lb, rb, rb], axis=0), preferred_element_type=F32
            )
            window = total[r * rows : (r + 1) * rows] + more
            out[0, b, r * rows : (r + 1) * rows, :] = cells[r * rows : (r + 1) * rows] / (
                floor + window * inverse
            )

    range_compress(0)
    pl.semaphore_wait(barrier, len(peers) + 1)
    for step in (1, -1):
        pl.semaphore_signal(ready, inc=1, device_id=dev(at(step * HOP, core)), device_id_type=MESH)
    start_by_place(0, 1, HOP)
    for b in range(1, beams):
        range_compress(b)
    pl.semaphore_wait(ready, 2)
    start_by_place(0, HOP + 1, chips // 2)
    for b in range(1, beams):
        start_by_place(b, 1, chips // 2)
    for l in range(pulses):
        for i in range(2):
            col = i * pulses + l
            dop[i, :, l * GB : (l + 1) * GB] = jnp.broadcast_to(tw[2, :, col : col + 1], (GA, GB))
    for b in range(beams):
        wait_blocks(recv_sem.at[b], size - 1)
        doppler(b)
        cfar(b)
    for b in range(beams):
        wait_blocks(own_sem.at[b], size - 1)


def solution(mesh):
    size = mesh.shape["shard"]

    def step(echoes, waveform, taper, guard, train, noise):
        _, _, beams, pulses, gates = echoes.shape
        depth = pulses * size
        tab_a, tab_b, twid = tables(depth)
        hbm = pl.BlockSpec(memory_space=pl.ANY)
        smem = pl.BlockSpec(memory_space=pltpu.SMEM)
        vmem = pltpu.VMEM
        dma = pltpu.SemaphoreType.DMA
        return pl.pallas_call(
            functools.partial(kernel, size),
            out_shape=jax.ShapeDtypeStruct((1, beams, depth, GB), F32),
            in_specs=[hbm, hbm, smem, smem, smem, smem, hbm, hbm, hbm],
            out_specs=pl.BlockSpec(memory_space=vmem),
            scratch_shapes=[
                vmem((beams, 2, pulses, gates), F32),
                vmem((2, gates), F32),
                vmem(tab_a.shape, BF16),
                vmem(tab_b.shape, BF16),
                vmem(twid.shape, F32),
                vmem((2, GA * pulses, GB), F32),
                vmem((GB, GB), F32),
                vmem((2, GA, GB), F32),
                vmem((beams, 2, depth, GB), F32),
                vmem((beams, 2, depth, GB), F32),
                vmem((2, GA, pulses * GB), F32),
                vmem((beams, depth, GB), F32),
                vmem((beams, 2, depth // 4, GB), F32),
                vmem((beams, 2, depth // 4, GB), F32),
                dma((4 + beams,)),
                dma((beams,)),
                dma((beams,)),
                pltpu.SemaphoreType.REGULAR,
                dma((beams, 2)),
                dma((beams, 2)),
            ],
            compiler_params=pltpu.CompilerParams(
                collective_id=0, has_side_effects=True, vmem_limit_bytes=56 * 2**20
            ),
            name="pulse_doppler",
        )(echoes, waveform, taper, guard, train, noise, jnp.asarray(tab_a), jnp.asarray(tab_b), jnp.asarray(twid))

    in_specs = (
        P(None, None, "groups", "shard", None),
        P(),
        P(),
        P("groups"),
        P("groups"),
        P("groups"),
    )
    out_specs = P(None, "groups", None, "shard")
    return jax.shard_map(step, mesh=mesh, in_specs=in_specs, out_specs=out_specs, check_vma=False)
```

```python
import functools
import math

import jax
import jax.numpy as jnp
import numpy as np
from jax import lax
from jax.experimental import pallas as pl
from jax.experimental.pallas import tpu as pltpu
from jax.sharding import PartitionSpec as P

MESH = pl.DeviceIdType.MESH
GA = 64
GB = 128
HALO = 20
HOP = 8
NEAR = 2
F32 = jnp.float32
BF16 = jnp.bfloat16


def split_host(table):
    high = table.astype(np.float32).astype(jnp.bfloat16)
    low = (table - high.astype(np.float64)).astype(np.float32).astype(jnp.bfloat16)
    return high, low


def tables(pulses):
    a = np.arange(GA)
    n = np.arange(GB)
    c = np.concatenate([np.arange(0, GB, 2), np.arange(1, GB, 2)])
    ang_a = 2 * math.pi / GA * (np.outer(a, a) % GA)
    ang_b = 2 * math.pi / GB * (np.outer(n, c) % GB)
    ca, sa = np.cos(ang_a), np.sin(ang_a)
    cb, sb = np.cos(ang_b), np.sin(ang_b)
    fwd_a = np.block([[ca, sa], [-sa, ca]])
    inv_a = np.block([[ca, -sa], [sa, ca]])
    fwd_b = np.block([[cb, -sb], [sb, cb]])
    inv_b = np.block([[cb.T, sb.T], [-sb.T, cb.T]])

    def left(m):
        h, l = split_host(m)
        return np.concatenate([h, h, l], axis=1)

    def right(m):
        h, l = split_host(m)
        return np.concatenate([h, h, l], axis=0)

    ang_t = 2 * math.pi / (GA * GB) * (np.outer(a, n) % (GA * GB))
    radix = pulses // GA
    ang_d = 2 * math.pi / pulses * (np.outer(a, np.arange(radix)) % pulses)
    small = np.zeros((GA, GB))
    small[:, :radix] = np.cos(ang_d)
    small[:, radix : 2 * radix] = np.sin(ang_d)
    twid = np.stack([np.cos(ang_t), np.sin(ang_t), small]).astype(np.float32)
    return (
        np.stack([left(fwd_a), left(inv_a)]),
        np.stack([right(fwd_b), right(inv_b)]),
        twid,
    )


def split(x):
    high = x.astype(BF16)
    return high, (x - high.astype(F32)).astype(BF16)


def dot_left(table, values):
    high, low = split(values)
    return jnp.dot(table, jnp.concatenate([high, low, high], axis=0), preferred_element_type=F32)


def dot_right(values, table):
    high, low = split(values)
    return jnp.dot(jnp.concatenate([high, low, high], axis=1), table, preferred_element_type=F32)


def compress(rows_re, rows_im, fwd_a, inv_a, fwd_b, inv_b, tc, ts, fr, fi):
    count = len(rows_re)
    x = jnp.concatenate(
        [jnp.concatenate(rows_re, axis=1), jnp.concatenate(rows_im, axis=1)], axis=0
    )
    y = dot_left(fwd_a, x)
    parts = []
    for p in range(count):
        yr = y[:GA, p * GB : (p + 1) * GB]
        yi = y[GA:, p * GB : (p + 1) * GB]
        parts.append(jnp.concatenate([yr * tc + yi * ts, yi * tc - yr * ts], axis=1))
    z = dot_right(jnp.concatenate(parts, axis=0), fwd_b)
    parts = []
    for p in range(count):
        zr = z[p * GA : (p + 1) * GA, :GB]
        zi = z[p * GA : (p + 1) * GA, GB:]
        parts.append(jnp.concatenate([zr * fr + zi * fi, zi * fr - zr * fi], axis=1))
    v = dot_right(jnp.concatenate(parts, axis=0), inv_b)
    re, im = [], []
    for p in range(count):
        vr = v[p * GA : (p + 1) * GA, :GB]
        vi = v[p * GA : (p + 1) * GA, GB:]
        re.append(vr * tc - vi * ts)
        im.append(vr * ts + vi * tc)
    return dot_left(
        inv_a,
        jnp.concatenate([jnp.concatenate(re, axis=1), jnp.concatenate(im, axis=1)], axis=0),
    )


def butterfly8(xs):
    r = math.sqrt(0.5)

    def add(u, v):
        return u[0] + v[0], u[1] + v[1]

    def sub(u, v):
        return u[0] - v[0], u[1] - v[1]

    def dft4(q):
        s02, d02 = add(q[0], q[2]), sub(q[0], q[2])
        s13, d13 = add(q[1], q[3]), sub(q[1], q[3])
        turned = (d13[1], -d13[0])
        return [add(s02, s13), add(d02, turned), sub(s02, s13), sub(d02, turned)]

    even, odd = dft4(xs[0::2]), dft4(xs[1::2])
    o1 = ((odd[1][0] + odd[1][1]) * r, (odd[1][1] - odd[1][0]) * r)
    o2 = (odd[2][1], -odd[2][0])
    o3 = ((odd[3][1] - odd[3][0]) * r, -(odd[3][0] + odd[3][1]) * r)
    odd = [odd[0], o1, o2, o3]
    return [add(even[k], odd[k]) for k in range(4)] + [sub(even[k], odd[k]) for k in range(4)]


def doppler_power(rows_re, rows_im, fwd_a, turn):
    count = len(rows_re)
    x = jnp.concatenate(
        [jnp.concatenate(rows_re, axis=1), jnp.concatenate(rows_im, axis=1)], axis=0
    )
    y = dot_left(fwd_a, x)
    terms = []
    for l in range(count):
        yr = y[:GA, l * GB : (l + 1) * GB]
        yi = y[GA:, l * GB : (l + 1) * GB]
        if l == 0:
            terms.append((yr, yi))
        else:
            dc, ds = turn(l)
            terms.append((yr * dc + yi * ds, yi * dc - yr * ds))
    return jnp.concatenate([r * r + i * i for r, i in butterfly8(terms)], axis=0)


def filter_grid(grid):
    turned = grid.T
    top, bottom = turned[:GA], turned[GA:]
    low = lax.broadcasted_iota(jnp.int32, (GA, GB), 1) < GA
    fr = jnp.where(low, top, pltpu.roll(bottom, GA, 1))
    fi = jnp.where(low, pltpu.roll(top, GA, 1), bottom)
    return fr, fi


def bands(guard, train):
    i = lax.broadcasted_iota(jnp.int32, (GB, GB), 0)
    j = lax.broadcasted_iota(jnp.int32, (GB, GB), 1)

    def inside(d):
        return jnp.where((d > guard) & (d <= guard + train), 1.0, 0.0).astype(F32)

    own = inside(jnp.abs(i - j))
    slot = lax.rem(i, 32)
    used = jnp.where(slot < HALO, 1.0, 0.0).astype(F32)
    left = inside(j + HALO - slot) * used
    right = inside(slot + GB - j) * used
    return own, left, right


def pack(power, lo):
    rows = power.shape[0] // 4
    lane = lax.broadcasted_iota(jnp.int32, (rows, GB), 1)
    out = None
    for r in range(4):
        block = power[r * rows : (r + 1) * rows]
        shift = (32 * r - lo) % GB
        moved = pltpu.roll(block, shift, 1) if shift else block
        out = moved if out is None else jnp.where(lane >= 32 * r, moved, out)
    return out


def kernel(
    size,
    echoes,
    waveform,
    taper,
    guard,
    train,
    noise,
    tab_a,
    tab_b,
    twid,
    out,
    x_in,
    w_in,
    ta,
    tb,
    tw,
    x_rows,
    grid,
    filt,
    own,
    recv,
    dop,
    power,
    window,
    halo_out,
    halo_in,
    in_sem,
    own_sem,
    recv_sem,
    ready,
    hs_sem,
    hr_sem,
):
    chips = size // 2
    me = lax.axis_index("shard")
    chip = lax.div(me, 2)
    core = lax.rem(me, 2)
    beams = echoes.shape[2]
    pulses = echoes.shape[3]
    depth = pulses * size

    def at(offset, k):
        return lax.rem(chip + offset + chips, chips) * 2 + k

    def dev(i):
        return {"shard": i}

    partner = chip * 2 + 1 - core

    loads = {}

    def load(name, src, dst, i):
        loads[name] = pltpu.make_async_copy(src, dst, in_sem.at[i])
        loads[name].start()

    load("x0", echoes.at[0, :, 0], x_in.at[0], 0)
    load("ta", tab_a, ta, 1)
    load("tw", twid, tw, 2)
    load("tb", tab_b, tb, 3)
    load("w", waveform, w_in, 4)
    for b in range(1, beams):
        load(f"x{b}", echoes.at[0, :, b], x_in.at[b], 4 + b)

    half = chips // 2
    first_half = chip < half

    barrier = pltpu.get_barrier_semaphore()

    def greet(offsets):
        for d in offsets:
            for k in range(2):
                pl.semaphore_signal(barrier, inc=1, device_id=dev(at(d, k)), device_id_type=MESH)

    wide = [d for d in range(-HOP, HOP + 1) if abs(d) > NEAR]
    pl.semaphore_signal(barrier, inc=1, device_id=dev(partner), device_id_type=MESH)
    greet([d for d in range(-NEAR, NEAR + 1) if d])
    pl.when(first_half)(lambda: greet(wide))
    greeters = 1 + 4 * NEAR
    for d in wide:
        greeters += jnp.where(lax.rem(chip + d + chips, chips) < half, 2, 0)

    def range_compress(b):
        loads[f"x{b}"].wait()
        for ri in range(2):
            for j in range(GA):
                x_rows[ri, j * pulses : (j + 1) * pulses, :] = x_in[b, ri, :, j * GB : (j + 1) * GB]
        if b == 0:
            loads["w"].wait()
            for ri in range(2):
                for j in range(GA):
                    grid[ri * GA + j : ri * GA + j + 1, :] = w_in[ri : ri + 1, j * GB : (j + 1) * GB]
            fr, fi = filter_grid(grid[...])
            filt[0] = fr
            filt[1] = fi
            for name in ("ta", "tw", "tb"):
                loads[name].wait()
        rows = [
            [x_rows[ri, pl.ds(p, GA, stride=pulses), :] for p in range(pulses)] for ri in range(2)
        ]
        done = compress(
            rows[0], rows[1], ta[0], ta[1], tb[0], tb[1], tw[0], tw[1], filt[0], filt[1]
        )
        scale = 1.0 / (GA * GB * math.sqrt(depth))
        for p in range(pulses):
            weight = taper[me * pulses + p] * scale
            for ri in range(2):
                own[b, ri, pl.ds(p, GA, stride=pulses), :] = (
                    done[ri * GA : (ri + 1) * GA, p * GB : (p + 1) * GB] * weight
                )
        mine = pl.ds(pl.multiple_of(me * pulses, pulses), pulses)
        recv[b, :, mine, :] = own[b, :, mine, :]

    def rows_of(i, n=1):
        return pl.ds(pl.multiple_of(i * pulses, pulses), n * pulses)

    def direct(b, to):
        return pltpu.make_async_remote_copy(
            src_ref=own.at[b, :, rows_of(to)],
            dst_ref=recv.at[b, :, rows_of(me)],
            send_sem=own_sem.at[b],
            recv_sem=recv_sem.at[b],
            device_id=dev(to),
            device_id_type=MESH,
        )

    def start_by_place(b, lo, hi, to=None):
        def both(offset):
            for k in range(2):
                direct(b, at(offset, k)).start()

        def when(condition, offset):
            pl.when(condition)(lambda: both(offset))

        def early():
            for m in range(1, half):
                if lo <= m <= hi:
                    if to is None:
                        both(m)
                    elif to == 0:
                        when(chip + m < half, m)
                    else:
                        when(chip + m >= half, m)
                if lo <= half - m <= hi and to != 1:
                    when(half - m <= chip, m - half)
            for m in range(half - 1, 0, -1):
                if lo <= m <= hi and to != 0:
                    when(m > chip, -m)
            if hi >= half:
                both(half)

        def late():
            if hi >= half:
                both(half)
            if to != 1:
                for place in range(half):
                    up = chips - chip + place
                    when((up >= lo) & (up <= min(hi, half - 1)), up)
                    down = chip - place
                    when((down >= lo) & (down <= min(hi, half - 1)), -down)
            if to != 0:
                for m in range(half - 1, 0, -1):
                    if lo <= m <= hi:
                        when(chip + m < chips, m)
                        when(chip - m >= half, -m)

        pl.when(first_half)(early)
        pl.when(jnp.logical_not(first_half))(late)

    def tell(step):
        for sign in (1, -1):
            pl.semaphore_signal(
                ready.at[step], inc=1, device_id=dev(at(sign * (NEAR << step), core)), device_id_type=MESH
            )

    def wait_blocks(sem, n):
        ref = own.at[0, :, pl.ds(0, n * pulses)]
        pltpu.make_async_copy(ref, ref, sem).wait()

    inner = (me > 0, me < size - 1)

    def halo_copy(b, side):
        to = lax.rem(me + (1 if side else size - 1), size)
        return pltpu.make_async_remote_copy(
            src_ref=halo_out.at[b, side],
            dst_ref=halo_in.at[b, 1 - side],
            send_sem=hs_sem.at[b, side],
            recv_sem=hr_sem.at[b, 1 - side],
            device_id=dev(to),
            device_id_type=MESH,
        )

    def doppler(b):
        rows = [
            [recv[b, ri, pl.ds(l, size, stride=pulses), :] for l in range(pulses)] for ri in range(2)
        ]
        value = doppler_power(
            rows[0], rows[1], ta[0], lambda l: (dop[0, :, l * GB : (l + 1) * GB], dop[1, :, l * GB : (l + 1) * GB])
        )
        halo_out[b, 0] = pack(value, 0)
        halo_out[b, 1] = pack(value, GB - HALO)
        power[b] = value
        for side in range(2):
            pl.when(inner[side])(halo_copy(b, side).start)

    def cfar_inside(b):
        high, low = split(power[b])
        band = bands(guard[b], train[b])[0].astype(BF16)
        window[b] = jnp.dot(
            jnp.concatenate([high, low], axis=1),
            jnp.concatenate([band, band], axis=0),
            preferred_element_type=F32,
        )

    def cfar(b):
        _, left_band, right_band = bands(guard[b], train[b])
        slot = lax.div(lax.broadcasted_iota(jnp.int32, (GB, GB), 0), 32)
        rows = depth // 4
        for side in range(2):

            def arrived():
                halo_copy(b, side).wait_send()
                halo_copy(b, 1 - side).wait_recv()

            def outside():
                halo_in[b, side] = jnp.zeros_like(halo_in[b, side])

            pl.when(inner[side])(arrived)
            pl.when(jnp.logical_not(inner[side]))(outside)
        left, right = halo_in[b, 0], halo_in[b, 1]
        lh, ll = split(left)
        rh, rl = split(right)
        edges = jnp.concatenate([lh, ll, rh, rl], axis=1)
        floor = noise[b]
        inverse = 1.0 / (2.0 * train[b].astype(F32))
        for r in range(4):
            lb = jnp.where(slot == r, left_band, 0.0).astype(BF16)
            rb = jnp.where(slot == r, right_band, 0.0).astype(BF16)
            more = jnp.dot(
                edges, jnp.concatenate([lb, lb, rb, rb], axis=0), preferred_element_type=F32
            )
            here = slice(r * rows, (r + 1) * rows)
            out[0, b, here, :] = power[b, here, :] / (floor + (window[b, here, :] + more) * inverse)

    range_compress(0)
    pl.semaphore_wait(barrier, greeters)
    tell(0)
    direct(0, partner).start()
    start_by_place(0, 1, NEAR)
    start_by_place(0, NEAR + 1, HOP, 0)
    for b in range(1, beams):
        range_compress(b)
    pl.semaphore_wait(ready.at[0], 2)
    tell(1)
    start_by_place(0, NEAR + 1, 2 * NEAR, 1)
    pl.semaphore_wait(ready.at[1], 2)
    tell(2)
    start_by_place(0, 2 * NEAR + 1, HOP, 1)
    pl.semaphore_wait(ready.at[2], 2)
    start_by_place(0, HOP + 1, half)
    for b in range(1, beams):
        direct(b, partner).start()
        start_by_place(b, 1, half)
    for l in range(pulses):
        for i in range(2):
            col = i * pulses + l
            dop[i, :, l * GB : (l + 1) * GB] = jnp.broadcast_to(tw[2, :, col : col + 1], (GA, GB))
    for b in range(beams):
        wait_blocks(recv_sem.at[b], size - 1)
        doppler(b)
        cfar_inside(b)
    for b in range(beams):
        cfar(b)
    for b in range(beams):
        wait_blocks(own_sem.at[b], size - 1)


def solution(mesh):
    size = mesh.shape["shard"]

    def step(echoes, waveform, taper, guard, train, noise):
        _, _, beams, pulses, gates = echoes.shape
        depth = pulses * size
        tab_a, tab_b, twid = tables(depth)
        hbm = pl.BlockSpec(memory_space=pl.ANY)
        smem = pl.BlockSpec(memory_space=pltpu.SMEM)
        vmem = pltpu.VMEM
        dma = pltpu.SemaphoreType.DMA
        return pl.pallas_call(
            functools.partial(kernel, size),
            out_shape=jax.ShapeDtypeStruct((1, beams, depth, GB), F32),
            in_specs=[hbm, hbm, smem, smem, smem, smem, hbm, hbm, hbm],
            out_specs=pl.BlockSpec(memory_space=vmem),
            scratch_shapes=[
                vmem((beams, 2, pulses, gates), F32),
                vmem((2, gates), F32),
                vmem(tab_a.shape, BF16),
                vmem(tab_b.shape, BF16),
                vmem(twid.shape, F32),
                vmem((2, GA * pulses, GB), F32),
                vmem((GB, GB), F32),
                vmem((2, GA, GB), F32),
                vmem((beams, 2, depth, GB), F32),
                vmem((beams, 2, depth, GB), F32),
                vmem((2, GA, pulses * GB), F32),
                vmem((beams, depth, GB), F32),
                vmem((beams, depth, GB), F32),
                vmem((beams, 2, depth // 4, GB), F32),
                vmem((beams, 2, depth // 4, GB), F32),
                dma((4 + beams,)),
                dma((beams,)),
                dma((beams,)),
                pltpu.SemaphoreType.REGULAR((3,)),
                dma((beams, 2)),
                dma((beams, 2)),
            ],
            compiler_params=pltpu.CompilerParams(
                collective_id=0, has_side_effects=True, vmem_limit_bytes=56 * 2**20
            ),
            name="pulse_doppler",
        )(echoes, waveform, taper, guard, train, noise, jnp.asarray(tab_a), jnp.asarray(tab_b), jnp.asarray(twid))

    in_specs = (
        P(None, None, "groups", "shard", None),
        P(),
        P(),
        P("groups"),
        P("groups"),
        P("groups"),
    )
    out_specs = P(None, "groups", None, "shard")
    return jax.shard_map(step, mesh=mesh, in_specs=in_specs, out_specs=out_specs, check_vma=False)
```

```python
import functools
import math

import jax
import jax.numpy as jnp
import numpy as np
from jax import lax
from jax.experimental import pallas as pl
from jax.experimental.pallas import tpu as pltpu
from jax.sharding import PartitionSpec as P

MESH = pl.DeviceIdType.MESH
GA = 64
GB = 128
HALO = 20
HOP = 8
NEAR = 2
F32 = jnp.float32
BF16 = jnp.bfloat16


def split_host(table):
    high = table.astype(np.float32).astype(jnp.bfloat16)
    low = (table - high.astype(np.float64)).astype(np.float32).astype(jnp.bfloat16)
    return high, low


def tables(pulses):
    a = np.arange(GA)
    n = np.arange(GB)
    c = np.concatenate([np.arange(0, GB, 2), np.arange(1, GB, 2)])
    ang_a = 2 * math.pi / GA * (np.outer(a, a) % GA)
    ang_b = 2 * math.pi / GB * (np.outer(n, c) % GB)
    ca, sa = np.cos(ang_a), np.sin(ang_a)
    cb, sb = np.cos(ang_b), np.sin(ang_b)
    fwd_a = np.block([[ca, sa], [-sa, ca]])
    inv_a = np.block([[ca, -sa], [sa, ca]])
    fwd_b = np.block([[cb, -sb], [sb, cb]])
    inv_b = np.block([[cb.T, sb.T], [-sb.T, cb.T]])

    def left(m):
        h, l = split_host(m)
        return np.concatenate([h, h, l], axis=1)

    def right(m):
        h, l = split_host(m)
        return np.concatenate([h, h, l], axis=0)

    ang_t = 2 * math.pi / (GA * GB) * (np.outer(a, n) % (GA * GB))
    radix = pulses // GA
    ang_d = 2 * math.pi / pulses * (np.outer(a, np.arange(radix)) % pulses)
    small = np.zeros((GA, GB))
    small[:, :radix] = np.cos(ang_d)
    small[:, radix : 2 * radix] = np.sin(ang_d)
    twid = np.stack([np.cos(ang_t), np.sin(ang_t), small]).astype(np.float32)
    return (
        np.stack([left(fwd_a), left(inv_a)]),
        np.stack([right(fwd_b), right(inv_b)]),
        twid,
    )


def split(x):
    high = x.astype(BF16)
    return high, (x - high.astype(F32)).astype(BF16)


def dot_left(table, values):
    high, low = split(values)
    return jnp.dot(table, jnp.concatenate([high, low, high], axis=0), preferred_element_type=F32)


def dot_right(values, table):
    high, low = split(values)
    return jnp.dot(jnp.concatenate([high, low, high], axis=1), table, preferred_element_type=F32)


def compress(rows_re, rows_im, fwd_a, inv_a, fwd_b, inv_b, tc, ts, fr, fi):
    count = len(rows_re)
    x = jnp.concatenate(
        [jnp.concatenate(rows_re, axis=1), jnp.concatenate(rows_im, axis=1)], axis=0
    )
    y = dot_left(fwd_a, x)
    parts = []
    for p in range(count):
        yr = y[:GA, p * GB : (p + 1) * GB]
        yi = y[GA:, p * GB : (p + 1) * GB]
        parts.append(jnp.concatenate([yr * tc + yi * ts, yi * tc - yr * ts], axis=1))
    z = dot_right(jnp.concatenate(parts, axis=0), fwd_b)
    parts = []
    for p in range(count):
        zr = z[p * GA : (p + 1) * GA, :GB]
        zi = z[p * GA : (p + 1) * GA, GB:]
        parts.append(jnp.concatenate([zr * fr + zi * fi, zi * fr - zr * fi], axis=1))
    v = dot_right(jnp.concatenate(parts, axis=0), inv_b)
    re, im = [], []
    for p in range(count):
        vr = v[p * GA : (p + 1) * GA, :GB]
        vi = v[p * GA : (p + 1) * GA, GB:]
        re.append(vr * tc - vi * ts)
        im.append(vr * ts + vi * tc)
    return dot_left(
        inv_a,
        jnp.concatenate([jnp.concatenate(re, axis=1), jnp.concatenate(im, axis=1)], axis=0),
    )


def butterfly8(xs):
    r = math.sqrt(0.5)

    def add(u, v):
        return u[0] + v[0], u[1] + v[1]

    def sub(u, v):
        return u[0] - v[0], u[1] - v[1]

    def dft4(q):
        s02, d02 = add(q[0], q[2]), sub(q[0], q[2])
        s13, d13 = add(q[1], q[3]), sub(q[1], q[3])
        turned = (d13[1], -d13[0])
        return [add(s02, s13), add(d02, turned), sub(s02, s13), sub(d02, turned)]

    even, odd = dft4(xs[0::2]), dft4(xs[1::2])
    o1 = ((odd[1][0] + odd[1][1]) * r, (odd[1][1] - odd[1][0]) * r)
    o2 = (odd[2][1], -odd[2][0])
    o3 = ((odd[3][1] - odd[3][0]) * r, -(odd[3][0] + odd[3][1]) * r)
    odd = [odd[0], o1, o2, o3]
    return [add(even[k], odd[k]) for k in range(4)] + [sub(even[k], odd[k]) for k in range(4)]


def doppler_power(rows_re, rows_im, fwd_a, turn):
    count = len(rows_re)
    x = jnp.concatenate(
        [jnp.concatenate(rows_re, axis=1), jnp.concatenate(rows_im, axis=1)], axis=0
    )
    y = dot_left(fwd_a, x)
    terms = []
    for l in range(count):
        yr = y[:GA, l * GB : (l + 1) * GB]
        yi = y[GA:, l * GB : (l + 1) * GB]
        if l == 0:
            terms.append((yr, yi))
        else:
            dc, ds = turn(l)
            terms.append((yr * dc + yi * ds, yi * dc - yr * ds))
    return jnp.concatenate([r * r + i * i for r, i in butterfly8(terms)], axis=0)


def filter_grid(grid):
    turned = grid.T
    top, bottom = turned[:GA], turned[GA:]
    low = lax.broadcasted_iota(jnp.int32, (GA, GB), 1) < GA
    fr = jnp.where(low, top, pltpu.roll(bottom, GA, 1))
    fi = jnp.where(low, pltpu.roll(top, GA, 1), bottom)
    return fr, fi


def bands(guard, train):
    i = lax.broadcasted_iota(jnp.int32, (GB, GB), 0)
    j = lax.broadcasted_iota(jnp.int32, (GB, GB), 1)

    def inside(d):
        return jnp.where((d > guard) & (d <= guard + train), 1.0, 0.0).astype(F32)

    own = inside(jnp.abs(i - j))
    slot = lax.rem(i, 32)
    used = jnp.where(slot < HALO, 1.0, 0.0).astype(F32)
    left = inside(j + HALO - slot) * used
    right = inside(slot + GB - j) * used
    return own, left, right


def pack(power, lo):
    rows = power.shape[0] // 4
    lane = lax.broadcasted_iota(jnp.int32, (rows, GB), 1)
    out = None
    for r in range(4):
        block = power[r * rows : (r + 1) * rows]
        shift = (32 * r - lo) % GB
        moved = pltpu.roll(block, shift, 1) if shift else block
        out = moved if out is None else jnp.where(lane >= 32 * r, moved, out)
    return out


def kernel(
    size,
    echoes,
    waveform,
    taper,
    guard,
    train,
    noise,
    tab_a,
    tab_b,
    twid,
    out,
    x_in,
    w_in,
    ta,
    tb,
    tw,
    x_rows,
    grid,
    filt,
    own,
    recv,
    dop,
    power,
    window,
    halo_out,
    halo_in,
    in_sem,
    own_sem,
    recv_sem,
    ready,
    hs_sem,
    hr_sem,
):
    chips = size // 2
    me = lax.axis_index("shard")
    chip = lax.div(me, 2)
    core = lax.rem(me, 2)
    beams = echoes.shape[2]
    pulses = echoes.shape[3]
    depth = pulses * size

    def at(offset, k):
        return lax.rem(chip + offset + chips, chips) * 2 + k

    def dev(i):
        return {"shard": i}

    partner = chip * 2 + 1 - core

    loads = {}

    def load(name, src, dst, i):
        loads[name] = pltpu.make_async_copy(src, dst, in_sem.at[i])
        loads[name].start()

    load("x0", echoes.at[0, :, 0], x_in.at[0], 0)
    load("ta", tab_a, ta, 1)
    load("tw", twid, tw, 2)
    load("tb", tab_b, tb, 3)
    load("w", waveform, w_in, 4)
    for b in range(1, beams):
        load(f"x{b}", echoes.at[0, :, b], x_in.at[b], 4 + b)

    half = chips // 2
    first_half = chip < half

    barrier = pltpu.get_barrier_semaphore()

    def greet(offsets):
        for d in offsets:
            for k in range(2):
                pl.semaphore_signal(barrier, inc=1, device_id=dev(at(d, k)), device_id_type=MESH)

    wide = [d for d in range(-HOP, HOP + 1) if abs(d) > NEAR]
    pl.semaphore_signal(barrier, inc=1, device_id=dev(partner), device_id_type=MESH)
    greet([d for d in range(-NEAR, NEAR + 1) if d])
    pl.when(first_half)(lambda: greet(wide))
    greeters = 1 + 4 * NEAR
    for d in wide:
        greeters += jnp.where(lax.rem(chip + d + chips, chips) < half, 2, 0)

    def range_compress(b):
        loads[f"x{b}"].wait()
        for ri in range(2):
            for j in range(GA):
                x_rows[ri, j * pulses : (j + 1) * pulses, :] = x_in[b, ri, :, j * GB : (j + 1) * GB]
        if b == 0:
            loads["w"].wait()
            for ri in range(2):
                for j in range(GA):
                    grid[ri * GA + j : ri * GA + j + 1, :] = w_in[ri : ri + 1, j * GB : (j + 1) * GB]
            fr, fi = filter_grid(grid[...])
            filt[0] = fr
            filt[1] = fi
            for name in ("ta", "tw", "tb"):
                loads[name].wait()
        rows = [
            [x_rows[ri, pl.ds(p, GA, stride=pulses), :] for p in range(pulses)] for ri in range(2)
        ]
        done = compress(
            rows[0], rows[1], ta[0], ta[1], tb[0], tb[1], tw[0], tw[1], filt[0], filt[1]
        )
        scale = 1.0 / (GA * GB * math.sqrt(depth))
        for p in range(pulses):
            weight = taper[me * pulses + p] * scale
            for ri in range(2):
                own[b, ri, pl.ds(p, GA, stride=pulses), :] = (
                    done[ri * GA : (ri + 1) * GA, p * GB : (p + 1) * GB] * weight
                )
        mine = pl.ds(pl.multiple_of(me * pulses, pulses), pulses)
        recv[b, :, mine, :] = own[b, :, mine, :]

    def rows_of(i, n=1):
        return pl.ds(pl.multiple_of(i * pulses, pulses), n * pulses)

    def direct(b, to):
        return pltpu.make_async_remote_copy(
            src_ref=own.at[b, :, rows_of(to)],
            dst_ref=recv.at[b, :, rows_of(me)],
            send_sem=own_sem.at[b],
            recv_sem=recv_sem.at[b],
            device_id=dev(to),
            device_id_type=MESH,
        )

    def start_by_place(b, lo, hi, to=None):
        def both(offset):
            for k in range(2):
                direct(b, at(offset, k)).start()

        def when(condition, offset):
            pl.when(condition)(lambda: both(offset))

        def early():
            for m in range(1, half):
                if lo <= m <= hi:
                    if to is None:
                        both(m)
                    elif to == 0:
                        when(chip + m < half, m)
                    else:
                        when(chip + m >= half, m)
                if lo <= half - m <= hi and to != 1:
                    when(half - m <= chip, m - half)
            for m in range(half - 1, 0, -1):
                if lo <= m <= hi and to != 0:
                    when(m > chip, -m)
            if hi >= half:
                both(half)

        def late():
            if hi >= half:
                both(half)
            if to != 1:
                for place in range(half):
                    up = chips - chip + place
                    when((up >= lo) & (up <= min(hi, half - 1)), up)
                    down = chip - place
                    when((down >= lo) & (down <= min(hi, half - 1)), -down)
            if to != 0:
                for m in range(half - 1, 0, -1):
                    if lo <= m <= hi:
                        when(chip + m < chips, m)
                        when(chip - m >= half, -m)

        pl.when(first_half)(early)
        pl.when(jnp.logical_not(first_half))(late)

    def tell(step):
        for sign in (1, -1):
            pl.semaphore_signal(
                ready.at[step], inc=1, device_id=dev(at(sign * (NEAR << step), core)), device_id_type=MESH
            )

    def wait_blocks(sem, n):
        ref = own.at[0, :, pl.ds(0, n * pulses)]
        pltpu.make_async_copy(ref, ref, sem).wait()

    inner = (me > 0, me < size - 1)

    def halo_copy(b, side):
        to = lax.rem(me + (1 if side else size - 1), size)
        return pltpu.make_async_remote_copy(
            src_ref=halo_out.at[b, side],
            dst_ref=halo_in.at[b, 1 - side],
            send_sem=hs_sem.at[b, side],
            recv_sem=hr_sem.at[b, 1 - side],
            device_id=dev(to),
            device_id_type=MESH,
        )

    def doppler(b):
        rows = [
            [recv[b, ri, pl.ds(l, size, stride=pulses), :] for l in range(pulses)] for ri in range(2)
        ]
        value = doppler_power(
            rows[0], rows[1], ta[0], lambda l: (dop[0, :, l * GB : (l + 1) * GB], dop[1, :, l * GB : (l + 1) * GB])
        )
        halo_out[b, 0] = pack(value, 0)
        halo_out[b, 1] = pack(value, GB - HALO)
        power[b] = value
        for side in range(2):
            pl.when(inner[side])(halo_copy(b, side).start)

    def cfar_inside(b):
        high, low = split(power[b])
        band = bands(guard[b], train[b])[0].astype(BF16)
        window[b] = jnp.dot(
            jnp.concatenate([high, low], axis=1),
            jnp.concatenate([band, band], axis=0),
            preferred_element_type=F32,
        )

    def cfar(b):
        _, left_band, right_band = bands(guard[b], train[b])
        slot = lax.div(lax.broadcasted_iota(jnp.int32, (GB, GB), 0), 32)
        rows = depth // 4
        for side in range(2):

            def arrived():
                halo_copy(b, side).wait_send()
                halo_copy(b, 1 - side).wait_recv()

            def outside():
                halo_in[b, side] = jnp.zeros_like(halo_in[b, side])

            pl.when(inner[side])(arrived)
            pl.when(jnp.logical_not(inner[side]))(outside)
        left, right = halo_in[b, 0], halo_in[b, 1]
        lh, ll = split(left)
        rh, rl = split(right)
        edges = jnp.concatenate([lh, ll, rh, rl], axis=1)
        floor = noise[b]
        inverse = 1.0 / (2.0 * train[b].astype(F32))
        for r in range(4):
            lb = jnp.where(slot == r, left_band, 0.0).astype(BF16)
            rb = jnp.where(slot == r, right_band, 0.0).astype(BF16)
            more = jnp.dot(
                edges, jnp.concatenate([lb, lb, rb, rb], axis=0), preferred_element_type=F32
            )
            here = slice(r * rows, (r + 1) * rows)
            out[0, b, here, :] = power[b, here, :] / (floor + (window[b, here, :] + more) * inverse)

    range_compress(0)
    pl.semaphore_wait(barrier, greeters)
    tell(0)
    direct(0, partner).start()
    start_by_place(0, 1, NEAR)
    start_by_place(0, NEAR + 1, HOP, 0)
    for b in range(1, beams):
        range_compress(b)
    pl.semaphore_wait(ready.at[0], 2)
    tell(1)
    start_by_place(0, NEAR + 1, 2 * NEAR, 1)
    pl.semaphore_wait(ready.at[1], 2)
    tell(2)
    start_by_place(0, 2 * NEAR + 1, HOP, 1)
    pl.semaphore_wait(ready.at[2], 2)
    start_by_place(0, HOP + 1, half)
    for b in range(1, beams):
        direct(b, partner).start()
        start_by_place(b, 1, half)
    for l in range(pulses):
        for i in range(2):
            col = i * pulses + l
            dop[i, :, l * GB : (l + 1) * GB] = jnp.broadcast_to(tw[2, :, col : col + 1], (GA, GB))
    for b in range(beams):
        wait_blocks(recv_sem.at[b], size - 1)
        doppler(b)
        cfar_inside(b)
    for b in range(beams):
        cfar(b)
    for b in range(beams):
        wait_blocks(own_sem.at[b], size - 1)


def solution(mesh):
    size = mesh.shape["shard"]

    def step(echoes, waveform, taper, guard, train, noise):
        _, _, beams, pulses, gates = echoes.shape
        depth = pulses * size
        tab_a, tab_b, twid = tables(depth)
        hbm = pl.BlockSpec(memory_space=pl.ANY)
        smem = pl.BlockSpec(memory_space=pltpu.SMEM)
        vmem = pltpu.VMEM
        dma = pltpu.SemaphoreType.DMA
        return pl.pallas_call(
            functools.partial(kernel, size),
            out_shape=vmem((1, beams, depth, GB), F32),
            in_specs=[hbm, hbm, smem, smem, smem, smem, hbm, hbm, hbm],
            out_specs=pl.BlockSpec(memory_space=vmem),
            scratch_shapes=[
                vmem((beams, 2, pulses, gates), F32),
                vmem((2, gates), F32),
                vmem(tab_a.shape, BF16),
                vmem(tab_b.shape, BF16),
                vmem(twid.shape, F32),
                vmem((2, GA * pulses, GB), F32),
                vmem((GB, GB), F32),
                vmem((2, GA, GB), F32),
                vmem((beams, 2, depth, GB), F32),
                vmem((beams, 2, depth, GB), F32),
                vmem((2, GA, pulses * GB), F32),
                vmem((beams, depth, GB), F32),
                vmem((beams, depth, GB), F32),
                vmem((beams, 2, depth // 4, GB), F32),
                vmem((beams, 2, depth // 4, GB), F32),
                dma((4 + beams,)),
                dma((beams,)),
                dma((beams,)),
                pltpu.SemaphoreType.REGULAR((3,)),
                dma((beams, 2)),
                dma((beams, 2)),
            ],
            compiler_params=pltpu.CompilerParams(
                collective_id=0, has_side_effects=True, vmem_limit_bytes=56 * 2**20
            ),
            name="pulse_doppler",
        )(echoes, waveform, taper, guard, train, noise, jnp.asarray(tab_a), jnp.asarray(tab_b), jnp.asarray(twid))

    in_specs = (
        P(None, None, "groups", "shard", None),
        P(),
        P(),
        P("groups"),
        P("groups"),
        P("groups"),
    )
    out_specs = P(None, "groups", None, "shard")
    return jax.shard_map(step, mesh=mesh, in_specs=in_specs, out_specs=out_specs, check_vma=False)
```

```python
import functools
import math

import jax
import jax.numpy as jnp
import numpy as np
from jax import lax
from jax.experimental import pallas as pl
from jax.experimental.pallas import tpu as pltpu
from jax.sharding import PartitionSpec as P

MESH = pl.DeviceIdType.MESH
GA = 64
GB = 128
HALO = 20
HOP = 8
NEAR = 2
PAUSE = 10
HOLDERS = 24
F32 = jnp.float32
BF16 = jnp.bfloat16


def split_host(table):
    high = table.astype(np.float32).astype(jnp.bfloat16)
    low = (table - high.astype(np.float64)).astype(np.float32).astype(jnp.bfloat16)
    return high, low


def tables(pulses):
    a = np.arange(GA)
    n = np.arange(GB)
    c = np.concatenate([np.arange(0, GB, 2), np.arange(1, GB, 2)])
    ang_a = 2 * math.pi / GA * (np.outer(a, a) % GA)
    ang_b = 2 * math.pi / GB * (np.outer(n, c) % GB)
    ca, sa = np.cos(ang_a), np.sin(ang_a)
    cb, sb = np.cos(ang_b), np.sin(ang_b)
    fwd_a = np.block([[ca, sa], [-sa, ca]])
    inv_a = np.block([[ca, -sa], [sa, ca]])
    fwd_b = np.block([[cb, -sb], [sb, cb]])
    inv_b = np.block([[cb.T, sb.T], [-sb.T, cb.T]])

    def left(m):
        h, l = split_host(m)
        return np.concatenate([h, h, l], axis=1)

    def right(m):
        h, l = split_host(m)
        return np.concatenate([h, h, l], axis=0)

    ang_t = 2 * math.pi / (GA * GB) * (np.outer(a, n) % (GA * GB))
    radix = pulses // GA
    ang_d = 2 * math.pi / pulses * (np.outer(a, np.arange(radix)) % pulses)
    small = np.zeros((GA, GB))
    small[:, :radix] = np.cos(ang_d)
    small[:, radix : 2 * radix] = np.sin(ang_d)
    twid = np.stack([np.cos(ang_t), np.sin(ang_t), small]).astype(np.float32)
    return (
        np.stack([left(fwd_a), left(inv_a)]),
        np.stack([right(fwd_b), right(inv_b)]),
        twid,
    )


def split(x):
    high = x.astype(BF16)
    return high, (x - high.astype(F32)).astype(BF16)


def dot_left(table, values):
    high, low = split(values)
    return jnp.dot(table, jnp.concatenate([high, low, high], axis=0), preferred_element_type=F32)


def dot_right(values, table):
    high, low = split(values)
    return jnp.dot(jnp.concatenate([high, low, high], axis=1), table, preferred_element_type=F32)


def compress(rows_re, rows_im, fwd_a, inv_a, fwd_b, inv_b, tc, ts, fr, fi):
    count = len(rows_re)
    x = jnp.concatenate(
        [jnp.concatenate(rows_re, axis=1), jnp.concatenate(rows_im, axis=1)], axis=0
    )
    y = dot_left(fwd_a, x)
    parts = []
    for p in range(count):
        yr = y[:GA, p * GB : (p + 1) * GB]
        yi = y[GA:, p * GB : (p + 1) * GB]
        parts.append(jnp.concatenate([yr * tc + yi * ts, yi * tc - yr * ts], axis=1))
    z = dot_right(jnp.concatenate(parts, axis=0), fwd_b)
    parts = []
    for p in range(count):
        zr = z[p * GA : (p + 1) * GA, :GB]
        zi = z[p * GA : (p + 1) * GA, GB:]
        parts.append(jnp.concatenate([zr * fr + zi * fi, zi * fr - zr * fi], axis=1))
    v = dot_right(jnp.concatenate(parts, axis=0), inv_b)
    re, im = [], []
    for p in range(count):
        vr = v[p * GA : (p + 1) * GA, :GB]
        vi = v[p * GA : (p + 1) * GA, GB:]
        re.append(vr * tc - vi * ts)
        im.append(vr * ts + vi * tc)
    return dot_left(
        inv_a,
        jnp.concatenate([jnp.concatenate(re, axis=1), jnp.concatenate(im, axis=1)], axis=0),
    )


def butterfly8(xs):
    r = math.sqrt(0.5)

    def add(u, v):
        return u[0] + v[0], u[1] + v[1]

    def sub(u, v):
        return u[0] - v[0], u[1] - v[1]

    def dft4(q):
        s02, d02 = add(q[0], q[2]), sub(q[0], q[2])
        s13, d13 = add(q[1], q[3]), sub(q[1], q[3])
        turned = (d13[1], -d13[0])
        return [add(s02, s13), add(d02, turned), sub(s02, s13), sub(d02, turned)]

    even, odd = dft4(xs[0::2]), dft4(xs[1::2])
    o1 = ((odd[1][0] + odd[1][1]) * r, (odd[1][1] - odd[1][0]) * r)
    o2 = (odd[2][1], -odd[2][0])
    o3 = ((odd[3][1] - odd[3][0]) * r, -(odd[3][0] + odd[3][1]) * r)
    odd = [odd[0], o1, o2, o3]
    return [add(even[k], odd[k]) for k in range(4)] + [sub(even[k], odd[k]) for k in range(4)]


def doppler_power(rows_re, rows_im, fwd_a, turn):
    count = len(rows_re)
    x = jnp.concatenate(
        [jnp.concatenate(rows_re, axis=1), jnp.concatenate(rows_im, axis=1)], axis=0
    )
    y = dot_left(fwd_a, x)
    terms = []
    for l in range(count):
        yr = y[:GA, l * GB : (l + 1) * GB]
        yi = y[GA:, l * GB : (l + 1) * GB]
        if l == 0:
            terms.append((yr, yi))
        else:
            dc, ds = turn(l)
            terms.append((yr * dc + yi * ds, yi * dc - yr * ds))
    return jnp.concatenate([r * r + i * i for r, i in butterfly8(terms)], axis=0)


def filter_grid(grid):
    turned = grid.T
    top, bottom = turned[:GA], turned[GA:]
    low = lax.broadcasted_iota(jnp.int32, (GA, GB), 1) < GA
    fr = jnp.where(low, top, pltpu.roll(bottom, GA, 1))
    fi = jnp.where(low, pltpu.roll(top, GA, 1), bottom)
    return fr, fi


def bands(guard, train):
    i = lax.broadcasted_iota(jnp.int32, (GB, GB), 0)
    j = lax.broadcasted_iota(jnp.int32, (GB, GB), 1)

    def inside(d):
        return jnp.where((d > guard) & (d <= guard + train), 1.0, 0.0).astype(F32)

    own = inside(jnp.abs(i - j))
    slot = lax.rem(i, 32)
    used = jnp.where(slot < HALO, 1.0, 0.0).astype(F32)
    left = inside(j + HALO - slot) * used
    right = inside(slot + GB - j) * used
    return own, left, right


def pack(power, lo):
    rows = power.shape[0] // 4
    lane = lax.broadcasted_iota(jnp.int32, (rows, GB), 1)
    out = None
    for r in range(4):
        block = power[r * rows : (r + 1) * rows]
        shift = (32 * r - lo) % GB
        moved = pltpu.roll(block, shift, 1) if shift else block
        out = moved if out is None else jnp.where(lane >= 32 * r, moved, out)
    return out


def kernel(
    size,
    echoes,
    waveform,
    taper,
    guard,
    train,
    noise,
    tab_a,
    tab_b,
    twid,
    out,
    x_in,
    w_in,
    ta,
    tb,
    tw,
    x_rows,
    grid,
    filt,
    own,
    recv,
    dop,
    power,
    window,
    edge_band,
    halo_out,
    halo_in,
    in_sem,
    own_sem,
    recv_sem,
    ready,
    hs_sem,
    hr_sem,
):
    chips = size // 2
    me = lax.axis_index("shard")
    chip = lax.div(me, 2)
    core = lax.rem(me, 2)
    beams = echoes.shape[2]
    pulses = echoes.shape[3]
    depth = pulses * size

    def at(offset, k):
        return lax.rem(chip + offset + chips, chips) * 2 + k

    def dev(i):
        return {"shard": i}

    partner = chip * 2 + 1 - core

    loads = {}

    def load(name, src, dst, i):
        loads[name] = pltpu.make_async_copy(src, dst, in_sem.at[i])
        loads[name].start()

    load("x0", echoes.at[0, :, 0], x_in.at[0], 0)
    load("ta", tab_a, ta, 1)
    load("tw", twid, tw, 2)
    load("tb", tab_b, tb, 3)
    load("w", waveform, w_in, 4)
    for b in range(1, beams):
        load(f"x{b}", echoes.at[0, :, b], x_in.at[b], 4 + b)

    half = chips // 2
    first_half = chip < half

    barrier = pltpu.get_barrier_semaphore()

    def greet(offsets):
        for d in offsets:
            for k in range(2):
                pl.semaphore_signal(barrier, inc=1, device_id=dev(at(d, k)), device_id_type=MESH)

    wide = [d for d in range(-HOP, HOP + 1) if abs(d) > NEAR]
    pl.semaphore_signal(barrier, inc=1, device_id=dev(partner), device_id_type=MESH)
    greet([d for d in range(-NEAR, NEAR + 1) if d])
    pl.when(first_half)(lambda: greet(wide))
    greeters = 1 + 4 * NEAR
    for d in wide:
        greeters += jnp.where(lax.rem(chip + d + chips, chips) < half, 2, 0)

    def range_compress(b):
        loads[f"x{b}"].wait()
        for ri in range(2):
            for j in range(GA):
                x_rows[ri, j * pulses : (j + 1) * pulses, :] = x_in[b, ri, :, j * GB : (j + 1) * GB]
        if b == 0:
            loads["w"].wait()
            for ri in range(2):
                for j in range(GA):
                    grid[ri * GA + j : ri * GA + j + 1, :] = w_in[ri : ri + 1, j * GB : (j + 1) * GB]
            fr, fi = filter_grid(grid[...])
            filt[0] = fr
            filt[1] = fi
            for name in ("ta", "tw", "tb"):
                loads[name].wait()
        rows = [
            [x_rows[ri, pl.ds(p, GA, stride=pulses), :] for p in range(pulses)] for ri in range(2)
        ]
        done = compress(
            rows[0], rows[1], ta[0], ta[1], tb[0], tb[1], tw[0], tw[1], filt[0], filt[1]
        )
        scale = 1.0 / (GA * GB * math.sqrt(depth))
        for p in range(pulses):
            weight = taper[me * pulses + p] * scale
            for ri in range(2):
                own[b, ri, pl.ds(p, GA, stride=pulses), :] = (
                    done[ri * GA : (ri + 1) * GA, p * GB : (p + 1) * GB] * weight
                )
        mine = pl.ds(pl.multiple_of(me * pulses, pulses), pulses)
        recv[b, :, mine, :] = own[b, :, mine, :]

    def rows_of(i, n=1):
        return pl.ds(pl.multiple_of(i * pulses, pulses), n * pulses)

    def direct(b, to):
        return pltpu.make_async_remote_copy(
            src_ref=own.at[b, :, rows_of(to)],
            dst_ref=recv.at[b, :, rows_of(me)],
            send_sem=own_sem.at[b],
            recv_sem=recv_sem.at[b],
            device_id=dev(to),
            device_id_type=MESH,
        )

    def start_by_place(b, lo, hi, to=None, hold=False):
        def both(offset):
            for k in range(2):
                direct(b, at(offset, k)).start()

        def when(condition, offset):
            pl.when(condition)(lambda: both(offset))

        def early():
            for m in range(1, half):
                if lo <= m <= hi:
                    if to is None:
                        both(m)
                    elif to == 0:
                        when(chip + m < half, m)
                    else:
                        when(chip + m >= half, m)
                if lo <= half - m <= hi and to != 1:
                    when(half - m <= chip, m - half)
            for m in range(half - 1, 0, -1):
                if lo <= m <= hi and to != 0:
                    when(m > chip, -m)
            if hi >= half:
                both(half)

        def late():
            if hi >= half:
                both(half)
            if to != 1:
                for place in range(half):
                    up = chips - chip + place
                    inside = (up >= lo) & (up <= min(hi, half - 1))
                    if hold and place >= PAUSE:
                        inside &= chip < HOLDERS
                    when(inside, up)
                    down = chip - place
                    when((down >= lo) & (down <= min(hi, half - 1)), -down)
            if to != 0:
                for m in range(half - 1, 0, -1):
                    if lo <= m <= hi:
                        when(chip + m < chips, m)
                        when(chip - m >= half, -m)

        pl.when(first_half)(early)
        pl.when(jnp.logical_not(first_half))(late)

    def start_held(b):
        def both(offset):
            for k in range(2):
                direct(b, at(offset, k)).start()

        def last():
            for place in range(PAUSE, half):
                up = chips - chip + place
                pl.when(up < half)(lambda: both(up))

        pl.when(chip >= HOLDERS)(last)

    def tell(step):
        for sign in (1, -1):
            pl.semaphore_signal(
                ready.at[step], inc=1, device_id=dev(at(sign * (NEAR << step), core)), device_id_type=MESH
            )

    def wait_blocks(sem, n):
        ref = own.at[0, :, pl.ds(0, n * pulses)]
        pltpu.make_async_copy(ref, ref, sem).wait()

    inner = (me > 0, me < size - 1)

    def halo_copy(b, side):
        to = lax.rem(me + (1 if side else size - 1), size)
        return pltpu.make_async_remote_copy(
            src_ref=halo_out.at[b, side],
            dst_ref=halo_in.at[b, 1 - side],
            send_sem=hs_sem.at[b, side],
            recv_sem=hr_sem.at[b, 1 - side],
            device_id=dev(to),
            device_id_type=MESH,
        )

    def doppler(b):
        rows = [
            [recv[b, ri, pl.ds(l, size, stride=pulses), :] for l in range(pulses)] for ri in range(2)
        ]
        value = doppler_power(
            rows[0], rows[1], ta[0], lambda l: (dop[0, :, l * GB : (l + 1) * GB], dop[1, :, l * GB : (l + 1) * GB])
        )
        halo_out[b, 0] = pack(value, 0)
        halo_out[b, 1] = pack(value, GB - HALO)
        power[b] = value
        for side in range(2):
            pl.when(inner[side])(halo_copy(b, side).start)

    def cfar_inside(b):
        own_band, left_band, right_band = bands(guard[b], train[b])
        high, low = split(power[b])
        band = own_band.astype(BF16)
        window[b] = jnp.dot(
            jnp.concatenate([high, low], axis=1),
            jnp.concatenate([band, band], axis=0),
            preferred_element_type=F32,
        )
        slot = lax.div(lax.broadcasted_iota(jnp.int32, (GB, GB), 0), 32)
        for r in range(4):
            lb = jnp.where(slot == r, left_band, 0.0).astype(BF16)
            rb = jnp.where(slot == r, right_band, 0.0).astype(BF16)
            edge_band[b, r] = jnp.concatenate([lb, lb, rb, rb], axis=0)

    def cfar(b):
        rows = depth // 4
        for side in range(2):

            def arrived():
                halo_copy(b, side).wait_send()
                halo_copy(b, 1 - side).wait_recv()

            def outside():
                halo_in[b, side] = jnp.zeros_like(halo_in[b, side])

            pl.when(inner[side])(arrived)
            pl.when(jnp.logical_not(inner[side]))(outside)
        left, right = halo_in[b, 0], halo_in[b, 1]
        lh, ll = split(left)
        rh, rl = split(right)
        edges = jnp.concatenate([lh, ll, rh, rl], axis=1)
        floor = noise[b]
        inverse = 1.0 / (2.0 * train[b].astype(F32))
        for r in range(4):
            more = jnp.dot(edges, edge_band[b, r], preferred_element_type=F32)
            here = slice(r * rows, (r + 1) * rows)
            out[0, b, here, :] = power[b, here, :] / (floor + (window[b, here, :] + more) * inverse)

    range_compress(0)
    pl.semaphore_wait(barrier, greeters)
    tell(0)
    direct(0, partner).start()
    start_by_place(0, 1, NEAR)
    start_by_place(0, NEAR + 1, HOP, 0)
    for b in range(1, beams):
        range_compress(b)
    pl.semaphore_wait(ready.at[0], 2)
    tell(1)
    start_by_place(0, NEAR + 1, 2 * NEAR, 1)
    pl.semaphore_wait(ready.at[1], 2)
    tell(2)
    start_by_place(0, 2 * NEAR + 1, HOP, 1)
    pl.semaphore_wait(ready.at[2], 2)
    start_by_place(0, HOP + 1, half)
    for b in range(1, beams):
        direct(b, partner).start()
        start_by_place(b, 1, half, hold=True)
    for l in range(pulses):
        for i in range(2):
            col = i * pulses + l
            dop[i, :, l * GB : (l + 1) * GB] = jnp.broadcast_to(tw[2, :, col : col + 1], (GA, GB))
    for b in range(beams):
        wait_blocks(recv_sem.at[b], size - 1)
        doppler(b)
        cfar_inside(b)
        if b == 0:
            for other in range(1, beams):
                start_held(other)
    for b in range(beams):
        cfar(b)
    for b in range(beams):
        wait_blocks(own_sem.at[b], size - 1)


def solution(mesh):
    size = mesh.shape["shard"]

    def step(echoes, waveform, taper, guard, train, noise):
        _, _, beams, pulses, gates = echoes.shape
        depth = pulses * size
        tab_a, tab_b, twid = tables(depth)
        hbm = pl.BlockSpec(memory_space=pl.ANY)
        smem = pl.BlockSpec(memory_space=pltpu.SMEM)
        vmem = pltpu.VMEM
        dma = pltpu.SemaphoreType.DMA
        return pl.pallas_call(
            functools.partial(kernel, size),
            out_shape=vmem((1, beams, depth, GB), F32),
            in_specs=[hbm, hbm, smem, smem, smem, smem, hbm, hbm, hbm],
            out_specs=pl.BlockSpec(memory_space=vmem),
            scratch_shapes=[
                vmem((beams, 2, pulses, gates), F32),
                vmem((2, gates), F32),
                vmem(tab_a.shape, BF16),
                vmem(tab_b.shape, BF16),
                vmem(twid.shape, F32),
                vmem((2, GA * pulses, GB), F32),
                vmem((GB, GB), F32),
                vmem((2, GA, GB), F32),
                vmem((beams, 2, depth, GB), F32),
                vmem((beams, 2, depth, GB), F32),
                vmem((2, GA, pulses * GB), F32),
                vmem((beams, depth, GB), F32),
                vmem((beams, depth, GB), F32),
                vmem((beams, 4, 4 * GB, GB), BF16),
                vmem((beams, 2, depth // 4, GB), F32),
                vmem((beams, 2, depth // 4, GB), F32),
                dma((4 + beams,)),
                dma((beams,)),
                dma((beams,)),
                pltpu.SemaphoreType.REGULAR((3,)),
                dma((beams, 2)),
                dma((beams, 2)),
            ],
            compiler_params=pltpu.CompilerParams(
                collective_id=0, has_side_effects=True, vmem_limit_bytes=56 * 2**20
            ),
            name="pulse_doppler",
        )(echoes, waveform, taper, guard, train, noise, jnp.asarray(tab_a), jnp.asarray(tab_b), jnp.asarray(twid))

    in_specs = (
        P(None, None, "groups", "shard", None),
        P(),
        P(),
        P("groups"),
        P("groups"),
        P("groups"),
    )
    out_specs = P(None, "groups", None, "shard")
    return jax.shard_map(step, mesh=mesh, in_specs=in_specs, out_specs=out_specs, check_vma=False)
```

```python
import functools
import math

import jax
import jax.numpy as jnp
import numpy as np
from jax import lax
from jax.experimental import pallas as pl
from jax.experimental.pallas import tpu as pltpu
from jax.sharding import PartitionSpec as P

MESH = pl.DeviceIdType.MESH
GA = 64
GB = 128
HALO = 20
HOP = 8
NEAR = 2
PAUSE = 10
HOLDERS = 24
F32 = jnp.float32
BF16 = jnp.bfloat16


def split_host(table):
    high = table.astype(np.float32).astype(jnp.bfloat16)
    low = (table - high.astype(np.float64)).astype(np.float32).astype(jnp.bfloat16)
    return high, low


def tables(pulses):
    a = np.arange(GA)
    n = np.arange(GB)
    c = np.concatenate([np.arange(0, GB, 2), np.arange(1, GB, 2)])
    ang_a = 2 * math.pi / GA * (np.outer(a, a) % GA)
    ang_b = 2 * math.pi / GB * (np.outer(n, c) % GB)
    ca, sa = np.cos(ang_a), np.sin(ang_a)
    cb, sb = np.cos(ang_b), np.sin(ang_b)
    fwd_a = np.block([[ca, sa], [-sa, ca]])
    inv_a = np.block([[ca, -sa], [sa, ca]])
    fwd_b = np.block([[cb, -sb], [sb, cb]])
    inv_b = np.block([[cb.T, sb.T], [-sb.T, cb.T]])

    def left(m):
        h, l = split_host(m)
        return np.concatenate([h, h, l], axis=1)

    def right(m):
        h, l = split_host(m)
        return np.concatenate([h, h, l], axis=0)

    ang_t = 2 * math.pi / (GA * GB) * (np.outer(a, n) % (GA * GB))
    radix = pulses // GA
    ang_d = 2 * math.pi / pulses * (np.outer(a, np.arange(radix)) % pulses)
    small = np.zeros((GA, GB))
    small[:, :radix] = np.cos(ang_d)
    small[:, radix : 2 * radix] = np.sin(ang_d)
    twid = np.stack([np.cos(ang_t), np.sin(ang_t), small]).astype(np.float32)
    return (
        np.stack([left(fwd_a), left(inv_a)]),
        np.stack([right(fwd_b), right(inv_b)]),
        twid,
    )


def split(x):
    high = x.astype(BF16)
    return high, (x - high.astype(F32)).astype(BF16)


def dot_left(table, values):
    high, low = split(values)
    return jnp.dot(table, jnp.concatenate([high, low, high], axis=0), preferred_element_type=F32)


def dot_right(values, table):
    high, low = split(values)
    return jnp.dot(jnp.concatenate([high, low, high], axis=1), table, preferred_element_type=F32)


def compress(rows_re, rows_im, fwd_a, inv_a, fwd_b, inv_b, tc, ts, fr, fi):
    count = len(rows_re)
    x = jnp.concatenate(
        [jnp.concatenate(rows_re, axis=1), jnp.concatenate(rows_im, axis=1)], axis=0
    )
    y = dot_left(fwd_a, x)
    parts = []
    for p in range(count):
        yr = y[:GA, p * GB : (p + 1) * GB]
        yi = y[GA:, p * GB : (p + 1) * GB]
        parts.append(jnp.concatenate([yr * tc + yi * ts, yi * tc - yr * ts], axis=1))
    z = dot_right(jnp.concatenate(parts, axis=0), fwd_b)
    parts = []
    for p in range(count):
        zr = z[p * GA : (p + 1) * GA, :GB]
        zi = z[p * GA : (p + 1) * GA, GB:]
        parts.append(jnp.concatenate([zr * fr + zi * fi, zi * fr - zr * fi], axis=1))
    v = dot_right(jnp.concatenate(parts, axis=0), inv_b)
    re, im = [], []
    for p in range(count):
        vr = v[p * GA : (p + 1) * GA, :GB]
        vi = v[p * GA : (p + 1) * GA, GB:]
        re.append(vr * tc - vi * ts)
        im.append(vr * ts + vi * tc)
    return dot_left(
        inv_a,
        jnp.concatenate([jnp.concatenate(re, axis=1), jnp.concatenate(im, axis=1)], axis=0),
    )


def butterfly8(xs):
    r = math.sqrt(0.5)

    def add(u, v):
        return u[0] + v[0], u[1] + v[1]

    def sub(u, v):
        return u[0] - v[0], u[1] - v[1]

    def dft4(q):
        s02, d02 = add(q[0], q[2]), sub(q[0], q[2])
        s13, d13 = add(q[1], q[3]), sub(q[1], q[3])
        turned = (d13[1], -d13[0])
        return [add(s02, s13), add(d02, turned), sub(s02, s13), sub(d02, turned)]

    even, odd = dft4(xs[0::2]), dft4(xs[1::2])
    o1 = ((odd[1][0] + odd[1][1]) * r, (odd[1][1] - odd[1][0]) * r)
    o2 = (odd[2][1], -odd[2][0])
    o3 = ((odd[3][1] - odd[3][0]) * r, -(odd[3][0] + odd[3][1]) * r)
    odd = [odd[0], o1, o2, o3]
    return [add(even[k], odd[k]) for k in range(4)] + [sub(even[k], odd[k]) for k in range(4)]


def doppler_power(rows_re, rows_im, fwd_a, turn):
    count = len(rows_re)
    x = jnp.concatenate(
        [jnp.concatenate(rows_re, axis=1), jnp.concatenate(rows_im, axis=1)], axis=0
    )
    y = dot_left(fwd_a, x)
    terms = []
    for l in range(count):
        yr = y[:GA, l * GB : (l + 1) * GB]
        yi = y[GA:, l * GB : (l + 1) * GB]
        if l == 0:
            terms.append((yr, yi))
        else:
            dc, ds = turn(l)
            terms.append((yr * dc + yi * ds, yi * dc - yr * ds))
    return jnp.concatenate([r * r + i * i for r, i in butterfly8(terms)], axis=0)


def filter_grid(grid):
    turned = grid.T
    top, bottom = turned[:GA], turned[GA:]
    low = lax.broadcasted_iota(jnp.int32, (GA, GB), 1) < GA
    fr = jnp.where(low, top, pltpu.roll(bottom, GA, 1))
    fi = jnp.where(low, pltpu.roll(top, GA, 1), bottom)
    return fr, fi


def bands(guard, train):
    i = lax.broadcasted_iota(jnp.int32, (GB, GB), 0)
    j = lax.broadcasted_iota(jnp.int32, (GB, GB), 1)

    def inside(d):
        return jnp.where((d > guard) & (d <= guard + train), 1.0, 0.0).astype(F32)

    own = inside(jnp.abs(i - j))
    slot = lax.rem(i, 32)
    used = jnp.where(slot < HALO, 1.0, 0.0).astype(F32)
    left = inside(j + HALO - slot) * used
    right = inside(slot + GB - j) * used
    return own, left, right


def pack(power, lo):
    rows = power.shape[0] // 4
    lane = lax.broadcasted_iota(jnp.int32, (rows, GB), 1)
    out = None
    for r in range(4):
        block = power[r * rows : (r + 1) * rows]
        shift = (32 * r - lo) % GB
        moved = pltpu.roll(block, shift, 1) if shift else block
        out = moved if out is None else jnp.where(lane >= 32 * r, moved, out)
    return out


def kernel(
    size,
    echoes,
    waveform,
    taper,
    guard,
    train,
    noise,
    tab_a,
    tab_b,
    twid,
    out,
    x_in,
    w_in,
    ta,
    tb,
    tw,
    x_rows,
    grid,
    filt,
    own,
    recv,
    dop,
    power,
    window,
    edge_band,
    halo_out,
    halo_in,
    in_sem,
    own_sem,
    recv_sem,
    ready,
    hs_sem,
    hr_sem,
):
    chips = size // 2
    me = lax.axis_index("shard")
    chip = lax.div(me, 2)
    core = lax.rem(me, 2)
    beams = echoes.shape[2]
    pulses = echoes.shape[3]
    depth = pulses * size

    def at(offset, k):
        return lax.rem(chip + offset + chips, chips) * 2 + k

    def dev(i):
        return {"shard": i}

    partner = chip * 2 + 1 - core

    loads = {}

    def load(name, src, dst, i):
        loads[name] = pltpu.make_async_copy(src, dst, in_sem.at[i])
        loads[name].start()

    load("w", waveform, w_in, 4)
    load("x0", echoes.at[0, :, 0], x_in.at[0], 0)
    load("ta", tab_a, ta, 1)
    load("tw", twid, tw, 2)
    load("tb", tab_b, tb, 3)
    for b in range(1, beams):
        load(f"x{b}", echoes.at[0, :, b], x_in.at[b], 4 + b)

    half = chips // 2
    first_half = chip < half

    barrier = pltpu.get_barrier_semaphore()

    def greet(offsets):
        for d in offsets:
            for k in range(2):
                pl.semaphore_signal(barrier, inc=1, device_id=dev(at(d, k)), device_id_type=MESH)

    wide = [d for d in range(-HOP, HOP + 1) if abs(d) > NEAR]
    pl.semaphore_signal(barrier, inc=1, device_id=dev(partner), device_id_type=MESH)
    greet([d for d in range(-NEAR, NEAR + 1) if d])
    pl.when(first_half)(lambda: greet(wide))
    greeters = 1 + 4 * NEAR
    for d in wide:
        greeters += jnp.where(lax.rem(chip + d + chips, chips) < half, 2, 0)

    def range_compress(b):
        if b == 0:
            loads["w"].wait()
            for ri in range(2):
                for j in range(GA):
                    grid[ri * GA + j : ri * GA + j + 1, :] = w_in[ri : ri + 1, j * GB : (j + 1) * GB]
            fr, fi = filter_grid(grid[...])
            filt[0] = fr
            filt[1] = fi
        loads[f"x{b}"].wait()
        for ri in range(2):
            for j in range(GA):
                x_rows[ri, j * pulses : (j + 1) * pulses, :] = x_in[b, ri, :, j * GB : (j + 1) * GB]
        if b == 0:
            for name in ("ta", "tw", "tb"):
                loads[name].wait()
        rows = [
            [x_rows[ri, pl.ds(p, GA, stride=pulses), :] for p in range(pulses)] for ri in range(2)
        ]
        done = compress(
            rows[0], rows[1], ta[0], ta[1], tb[0], tb[1], tw[0], tw[1], filt[0], filt[1]
        )
        scale = 1.0 / (GA * GB * math.sqrt(depth))
        for p in range(pulses):
            weight = taper[me * pulses + p] * scale
            for ri in range(2):
                own[b, ri, pl.ds(p, GA, stride=pulses), :] = (
                    done[ri * GA : (ri + 1) * GA, p * GB : (p + 1) * GB] * weight
                )

    def keep_own(b):
        mine = pl.ds(pl.multiple_of(me * pulses, pulses), pulses)
        recv[b, :, mine, :] = own[b, :, mine, :]

    def rows_of(i, n=1):
        return pl.ds(pl.multiple_of(i * pulses, pulses), n * pulses)

    def direct(b, to):
        return pltpu.make_async_remote_copy(
            src_ref=own.at[b, :, rows_of(to)],
            dst_ref=recv.at[b, :, rows_of(me)],
            send_sem=own_sem.at[b],
            recv_sem=recv_sem.at[b],
            device_id=dev(to),
            device_id_type=MESH,
        )

    def start_by_place(b, lo, hi, to=None, hold=False):
        def both(offset):
            for k in range(2):
                direct(b, at(offset, k)).start()

        def when(condition, offset):
            pl.when(condition)(lambda: both(offset))

        def early():
            for m in range(1, half):
                if lo <= m <= hi:
                    if to is None:
                        both(m)
                    elif to == 0:
                        when(chip + m < half, m)
                    else:
                        when(chip + m >= half, m)
                if lo <= half - m <= hi and to != 1:
                    when(half - m <= chip, m - half)
            for m in range(half - 1, 0, -1):
                if lo <= m <= hi and to != 0:
                    when(m > chip, -m)
            if hi >= half:
                both(half)

        def late():
            if hi >= half:
                both(half)
            if to != 1:
                for place in range(half):
                    up = chips - chip + place
                    inside = (up >= lo) & (up <= min(hi, half - 1))
                    if hold and place >= PAUSE:
                        inside &= chip < HOLDERS
                    when(inside, up)
                    down = chip - place
                    when((down >= lo) & (down <= min(hi, half - 1)), -down)
            if to != 0:
                for m in range(half - 1, 0, -1):
                    if lo <= m <= hi:
                        when(chip + m < chips, m)
                        when(chip - m >= half, -m)

        pl.when(first_half)(early)
        pl.when(jnp.logical_not(first_half))(late)

    def start_held(b):
        def both(offset):
            for k in range(2):
                direct(b, at(offset, k)).start()

        def last():
            for place in range(PAUSE, half):
                up = chips - chip + place
                pl.when(up < half)(lambda: both(up))

        pl.when(chip >= HOLDERS)(last)

    def tell(step):
        for sign in (1, -1):
            pl.semaphore_signal(
                ready.at[step], inc=1, device_id=dev(at(sign * (NEAR << step), core)), device_id_type=MESH
            )

    def wait_blocks(sem, n):
        ref = own.at[0, :, pl.ds(0, n * pulses)]
        pltpu.make_async_copy(ref, ref, sem).wait()

    inner = (me > 0, me < size - 1)

    def halo_copy(b, side):
        to = lax.rem(me + (1 if side else size - 1), size)
        return pltpu.make_async_remote_copy(
            src_ref=halo_out.at[b, side],
            dst_ref=halo_in.at[b, 1 - side],
            send_sem=hs_sem.at[b, side],
            recv_sem=hr_sem.at[b, 1 - side],
            device_id=dev(to),
            device_id_type=MESH,
        )

    def doppler(b):
        rows = [
            [recv[b, ri, pl.ds(l, size, stride=pulses), :] for l in range(pulses)] for ri in range(2)
        ]
        value = doppler_power(
            rows[0], rows[1], ta[0], lambda l: (dop[0, :, l * GB : (l + 1) * GB], dop[1, :, l * GB : (l + 1) * GB])
        )
        halo_out[b, 0] = pack(value, 0)
        halo_out[b, 1] = pack(value, GB - HALO)
        power[b] = value
        for side in range(2):
            pl.when(inner[side])(halo_copy(b, side).start)

    def cfar_inside(b):
        own_band, left_band, right_band = bands(guard[b], train[b])
        high, low = split(power[b])
        band = own_band.astype(BF16)
        window[b] = jnp.dot(
            jnp.concatenate([high, low], axis=1),
            jnp.concatenate([band, band], axis=0),
            preferred_element_type=F32,
        )
        slot = lax.div(lax.broadcasted_iota(jnp.int32, (GB, GB), 0), 32)
        for r in range(4):
            lb = jnp.where(slot == r, left_band, 0.0).astype(BF16)
            rb = jnp.where(slot == r, right_band, 0.0).astype(BF16)
            edge_band[b, r] = jnp.concatenate([lb, lb, rb, rb], axis=0)

    def cfar(b):
        rows = depth // 4
        for side in range(2):

            def arrived():
                halo_copy(b, side).wait_send()
                halo_copy(b, 1 - side).wait_recv()

            def outside():
                halo_in[b, side] = jnp.zeros_like(halo_in[b, side])

            pl.when(inner[side])(arrived)
            pl.when(jnp.logical_not(inner[side]))(outside)
        left, right = halo_in[b, 0], halo_in[b, 1]
        lh, ll = split(left)
        rh, rl = split(right)
        edges = jnp.concatenate([lh, ll, rh, rl], axis=1)
        floor = noise[b]
        inverse = 1.0 / (2.0 * train[b].astype(F32))
        for r in range(4):
            more = jnp.dot(edges, edge_band[b, r], preferred_element_type=F32)
            here = slice(r * rows, (r + 1) * rows)
            out[0, b, here, :] = power[b, here, :] / (floor + (window[b, here, :] + more) * inverse)

    range_compress(0)
    pl.semaphore_wait(barrier, greeters)
    tell(0)
    direct(0, partner).start()
    start_by_place(0, 1, NEAR)
    start_by_place(0, NEAR + 1, HOP, 0)
    for b in range(1, beams):
        range_compress(b)
    pl.semaphore_wait(ready.at[0], 2)
    tell(1)
    start_by_place(0, NEAR + 1, 2 * NEAR, 1)
    pl.semaphore_wait(ready.at[1], 2)
    tell(2)
    start_by_place(0, 2 * NEAR + 1, HOP, 1)
    pl.semaphore_wait(ready.at[2], 2)
    start_by_place(0, HOP + 1, half)
    for b in range(1, beams):
        direct(b, partner).start()
        start_by_place(b, 1, half, hold=True)
    for b in range(beams):
        keep_own(b)
    for l in range(pulses):
        for i in range(2):
            col = i * pulses + l
            dop[i, :, l * GB : (l + 1) * GB] = jnp.broadcast_to(tw[2, :, col : col + 1], (GA, GB))
    for b in range(beams):
        wait_blocks(recv_sem.at[b], size - 1)
        doppler(b)
        cfar_inside(b)
        if b == 0:
            for other in range(1, beams):
                start_held(other)
    for b in range(beams):
        cfar(b)
    for b in range(beams):
        wait_blocks(own_sem.at[b], size - 1)


def solution(mesh):
    size = mesh.shape["shard"]

    def step(echoes, waveform, taper, guard, train, noise):
        _, _, beams, pulses, gates = echoes.shape
        depth = pulses * size
        tab_a, tab_b, twid = tables(depth)
        hbm = pl.BlockSpec(memory_space=pl.ANY)
        smem = pl.BlockSpec(memory_space=pltpu.SMEM)
        vmem = pltpu.VMEM
        dma = pltpu.SemaphoreType.DMA
        return pl.pallas_call(
            functools.partial(kernel, size),
            out_shape=vmem((1, beams, depth, GB), F32),
            in_specs=[hbm, hbm, smem, smem, smem, smem, hbm, hbm, hbm],
            out_specs=pl.BlockSpec(memory_space=vmem),
            scratch_shapes=[
                vmem((beams, 2, pulses, gates), F32),
                vmem((2, gates), F32),
                vmem(tab_a.shape, BF16),
                vmem(tab_b.shape, BF16),
                vmem(twid.shape, F32),
                vmem((2, GA * pulses, GB), F32),
                vmem((GB, GB), F32),
                vmem((2, GA, GB), F32),
                vmem((beams, 2, depth, GB), F32),
                vmem((beams, 2, depth, GB), F32),
                vmem((2, GA, pulses * GB), F32),
                vmem((beams, depth, GB), F32),
                vmem((beams, depth, GB), F32),
                vmem((beams, 4, 4 * GB, GB), BF16),
                vmem((beams, 2, depth // 4, GB), F32),
                vmem((beams, 2, depth // 4, GB), F32),
                dma((4 + beams,)),
                dma((beams,)),
                dma((beams,)),
                pltpu.SemaphoreType.REGULAR((3,)),
                dma((beams, 2)),
                dma((beams, 2)),
            ],
            compiler_params=pltpu.CompilerParams(
                collective_id=0, has_side_effects=True, vmem_limit_bytes=56 * 2**20
            ),
            name="pulse_doppler",
        )(echoes, waveform, taper, guard, train, noise, jnp.asarray(tab_a), jnp.asarray(tab_b), jnp.asarray(twid))

    in_specs = (
        P(None, None, "groups", "shard", None),
        P(),
        P(),
        P("groups"),
        P("groups"),
        P("groups"),
    )
    out_specs = P(None, "groups", None, "shard")
    return jax.shard_map(step, mesh=mesh, in_specs=in_specs, out_specs=out_specs, check_vma=False)
```

```python
import functools
import math

import jax
import jax.numpy as jnp
import numpy as np
from jax import lax
from jax.experimental import pallas as pl
from jax.experimental.pallas import tpu as pltpu
from jax.sharding import PartitionSpec as P

MESH = pl.DeviceIdType.MESH
GA = 64
GB = 128
HALO = 20
HOP = 8
NEAR = 2
PAUSE = 9
HOLDERS = 28
F32 = jnp.float32
BF16 = jnp.bfloat16


def split_host(table):
    high = table.astype(np.float32).astype(jnp.bfloat16)
    low = (table - high.astype(np.float64)).astype(np.float32).astype(jnp.bfloat16)
    return high, low


def tables(pulses):
    a = np.arange(GA)
    n = np.arange(GB)
    c = np.concatenate([np.arange(0, GB, 2), np.arange(1, GB, 2)])
    ang_a = 2 * math.pi / GA * (np.outer(a, a) % GA)
    ang_b = 2 * math.pi / GB * (np.outer(n, c) % GB)
    ca, sa = np.cos(ang_a), np.sin(ang_a)
    cb, sb = np.cos(ang_b), np.sin(ang_b)
    fwd_a = np.block([[ca, sa], [-sa, ca]])
    inv_a = np.block([[ca, -sa], [sa, ca]])
    fwd_b = np.block([[cb, -sb], [sb, cb]])
    inv_b = np.block([[cb.T, sb.T], [-sb.T, cb.T]])

    def left(m):
        h, l = split_host(m)
        return np.concatenate([h, h, l], axis=1)

    def right(m):
        h, l = split_host(m)
        return np.concatenate([h, h, l], axis=0)

    ang_t = 2 * math.pi / (GA * GB) * (np.outer(a, n) % (GA * GB))
    radix = pulses // GA
    ang_d = 2 * math.pi / pulses * (np.outer(a, np.arange(radix)) % pulses)
    small = np.zeros((GA, GB))
    small[:, :radix] = np.cos(ang_d)
    small[:, radix : 2 * radix] = np.sin(ang_d)
    twid = np.stack([np.cos(ang_t), np.sin(ang_t), small]).astype(np.float32)
    return (
        np.stack([left(fwd_a), left(inv_a)]),
        np.stack([right(fwd_b), right(inv_b)]),
        twid,
    )


def split(x):
    high = x.astype(BF16)
    return high, (x - high.astype(F32)).astype(BF16)


def dot_left(table, values):
    high, low = split(values)
    return jnp.dot(table, jnp.concatenate([high, low, high], axis=0), preferred_element_type=F32)


def dot_right(values, table):
    high, low = split(values)
    return jnp.dot(jnp.concatenate([high, low, high], axis=1), table, preferred_element_type=F32)


def compress(rows_re, rows_im, fwd_a, inv_a, fwd_b, inv_b, tc, ts, fr, fi):
    count = len(rows_re)
    x = jnp.concatenate(
        [jnp.concatenate(rows_re, axis=1), jnp.concatenate(rows_im, axis=1)], axis=0
    )
    y = dot_left(fwd_a, x)
    parts = []
    for p in range(count):
        yr = y[:GA, p * GB : (p + 1) * GB]
        yi = y[GA:, p * GB : (p + 1) * GB]
        parts.append(jnp.concatenate([yr * tc + yi * ts, yi * tc - yr * ts], axis=1))
    z = dot_right(jnp.concatenate(parts, axis=0), fwd_b)
    parts = []
    for p in range(count):
        zr = z[p * GA : (p + 1) * GA, :GB]
        zi = z[p * GA : (p + 1) * GA, GB:]
        parts.append(jnp.concatenate([zr * fr + zi * fi, zi * fr - zr * fi], axis=1))
    v = dot_right(jnp.concatenate(parts, axis=0), inv_b)
    re, im = [], []
    for p in range(count):
        vr = v[p * GA : (p + 1) * GA, :GB]
        vi = v[p * GA : (p + 1) * GA, GB:]
        re.append(vr * tc - vi * ts)
        im.append(vr * ts + vi * tc)
    return dot_left(
        inv_a,
        jnp.concatenate([jnp.concatenate(re, axis=1), jnp.concatenate(im, axis=1)], axis=0),
    )


def butterfly8(xs):
    r = math.sqrt(0.5)

    def add(u, v):
        return u[0] + v[0], u[1] + v[1]

    def sub(u, v):
        return u[0] - v[0], u[1] - v[1]

    def dft4(q):
        s02, d02 = add(q[0], q[2]), sub(q[0], q[2])
        s13, d13 = add(q[1], q[3]), sub(q[1], q[3])
        turned = (d13[1], -d13[0])
        return [add(s02, s13), add(d02, turned), sub(s02, s13), sub(d02, turned)]

    even, odd = dft4(xs[0::2]), dft4(xs[1::2])
    o1 = ((odd[1][0] + odd[1][1]) * r, (odd[1][1] - odd[1][0]) * r)
    o2 = (odd[2][1], -odd[2][0])
    o3 = ((odd[3][1] - odd[3][0]) * r, -(odd[3][0] + odd[3][1]) * r)
    odd = [odd[0], o1, o2, o3]
    return [add(even[k], odd[k]) for k in range(4)] + [sub(even[k], odd[k]) for k in range(4)]


def doppler_power(rows_re, rows_im, fwd_a, turn):
    count = len(rows_re)
    x = jnp.concatenate(
        [jnp.concatenate(rows_re, axis=1), jnp.concatenate(rows_im, axis=1)], axis=0
    )
    y = dot_left(fwd_a, x)
    terms = []
    for l in range(count):
        yr = y[:GA, l * GB : (l + 1) * GB]
        yi = y[GA:, l * GB : (l + 1) * GB]
        if l == 0:
            terms.append((yr, yi))
        else:
            dc, ds = turn(l)
            terms.append((yr * dc + yi * ds, yi * dc - yr * ds))
    return jnp.concatenate([r * r + i * i for r, i in butterfly8(terms)], axis=0)


def filter_grid(grid):
    turned = grid.T
    top, bottom = turned[:GA], turned[GA:]
    low = lax.broadcasted_iota(jnp.int32, (GA, GB), 1) < GA
    fr = jnp.where(low, top, pltpu.roll(bottom, GA, 1))
    fi = jnp.where(low, pltpu.roll(top, GA, 1), bottom)
    return fr, fi


def bands(guard, train):
    i = lax.broadcasted_iota(jnp.int32, (GB, GB), 0)
    j = lax.broadcasted_iota(jnp.int32, (GB, GB), 1)

    def inside(d):
        return jnp.where((d > guard) & (d <= guard + train), 1.0, 0.0).astype(F32)

    own = inside(jnp.abs(i - j))
    slot = lax.rem(i, 32)
    used = jnp.where(slot < HALO, 1.0, 0.0).astype(F32)
    left = inside(j + HALO - slot) * used
    right = inside(slot + GB - j) * used
    return own, left, right


def pack(power, lo):
    rows = power.shape[0] // 4
    lane = lax.broadcasted_iota(jnp.int32, (rows, GB), 1)
    out = None
    for r in range(4):
        block = power[r * rows : (r + 1) * rows]
        shift = (32 * r - lo) % GB
        moved = pltpu.roll(block, shift, 1) if shift else block
        out = moved if out is None else jnp.where(lane >= 32 * r, moved, out)
    return out


def kernel(
    size,
    echoes,
    waveform,
    taper,
    guard,
    train,
    noise,
    tab_a,
    tab_b,
    twid,
    out,
    x_in,
    w_in,
    ta,
    tb,
    tw,
    x_rows,
    grid,
    filt,
    own,
    recv,
    dop,
    power,
    window,
    edge_band,
    halo_out,
    halo_in,
    in_sem,
    own_sem,
    recv_sem,
    ready,
    hs_sem,
    hr_sem,
):
    chips = size // 2
    me = lax.axis_index("shard")
    chip = lax.div(me, 2)
    core = lax.rem(me, 2)
    beams = echoes.shape[2]
    pulses = echoes.shape[3]
    depth = pulses * size

    def at(offset, k):
        return lax.rem(chip + offset + chips, chips) * 2 + k

    def dev(i):
        return {"shard": i}

    partner = chip * 2 + 1 - core

    loads = {}

    def load(name, src, dst, i):
        loads[name] = pltpu.make_async_copy(src, dst, in_sem.at[i])
        loads[name].start()

    load("w", waveform, w_in, 4)
    load("x0", echoes.at[0, :, 0], x_in.at[0], 0)
    load("ta", tab_a, ta, 1)
    load("tw", twid, tw, 2)
    load("tb", tab_b, tb, 3)
    for b in range(1, beams):
        load(f"x{b}", echoes.at[0, :, b], x_in.at[b], 4 + b)

    half = chips // 2
    first_half = chip < half

    barrier = pltpu.get_barrier_semaphore()

    def greet(offsets):
        for d in offsets:
            for k in range(2):
                pl.semaphore_signal(barrier, inc=1, device_id=dev(at(d, k)), device_id_type=MESH)

    wide = [d for d in range(-HOP, HOP + 1) if abs(d) > NEAR]
    pl.semaphore_signal(barrier, inc=1, device_id=dev(partner), device_id_type=MESH)
    greet([d for d in range(-NEAR, NEAR + 1) if d])
    pl.when(first_half)(lambda: greet(wide))
    greeters = 1 + 4 * NEAR
    for d in wide:
        greeters += jnp.where(lax.rem(chip + d + chips, chips) < half, 2, 0)

    def range_compress(b):
        if b == 0:
            loads["w"].wait()
            for ri in range(2):
                for j in range(GA):
                    grid[ri * GA + j : ri * GA + j + 1, :] = w_in[ri : ri + 1, j * GB : (j + 1) * GB]
            fr, fi = filter_grid(grid[...])
            filt[0] = fr
            filt[1] = fi
        loads[f"x{b}"].wait()
        for ri in range(2):
            for j in range(GA):
                x_rows[ri, j * pulses : (j + 1) * pulses, :] = x_in[b, ri, :, j * GB : (j + 1) * GB]
        if b == 0:
            for name in ("ta", "tw", "tb"):
                loads[name].wait()
        rows = [
            [x_rows[ri, pl.ds(p, GA, stride=pulses), :] for p in range(pulses)] for ri in range(2)
        ]
        done = compress(
            rows[0], rows[1], ta[0], ta[1], tb[0], tb[1], tw[0], tw[1], filt[0], filt[1]
        )
        scale = 1.0 / (GA * GB * math.sqrt(depth))
        for p in range(pulses):
            weight = taper[me * pulses + p] * scale
            for ri in range(2):
                own[b, ri, pl.ds(p, GA, stride=pulses), :] = (
                    done[ri * GA : (ri + 1) * GA, p * GB : (p + 1) * GB] * weight
                )

    def keep_own(b):
        mine = pl.ds(pl.multiple_of(me * pulses, pulses), pulses)
        recv[b, :, mine, :] = own[b, :, mine, :]

    def rows_of(i, n=1):
        return pl.ds(pl.multiple_of(i * pulses, pulses), n * pulses)

    def direct(b, to):
        return pltpu.make_async_remote_copy(
            src_ref=own.at[b, :, rows_of(to)],
            dst_ref=recv.at[b, :, rows_of(me)],
            send_sem=own_sem.at[b],
            recv_sem=recv_sem.at[b],
            device_id=dev(to),
            device_id_type=MESH,
        )

    def start_by_place(b, lo, hi, to=None, hold=False):
        def both(offset):
            for k in range(2):
                direct(b, at(offset, k)).start()

        def when(condition, offset):
            pl.when(condition)(lambda: both(offset))

        def early():
            for m in range(1, half):
                if lo <= m <= hi:
                    if to is None:
                        both(m)
                    elif to == 0:
                        when(chip + m < half, m)
                    else:
                        when(chip + m >= half, m)
                if lo <= half - m <= hi and to != 1:
                    when(half - m <= chip, m - half)
            for m in range(half - 1, 0, -1):
                if lo <= m <= hi and to != 0:
                    when(m > chip, -m)
            if hi >= half:
                both(half)

        def late():
            if hi >= half:
                both(half)
            if to != 1:
                for place in range(half):
                    up = chips - chip + place
                    inside = (up >= lo) & (up <= min(hi, half - 1))
                    if hold and place >= PAUSE:
                        inside &= chip < HOLDERS
                    when(inside, up)
                    down = chip - place
                    when((down >= lo) & (down <= min(hi, half - 1)), -down)
            if to != 0:
                for m in range(half - 1, 0, -1):
                    if lo <= m <= hi:
                        when(chip + m < chips, m)
                        when(chip - m >= half, -m)

        pl.when(first_half)(early)
        pl.when(jnp.logical_not(first_half))(late)

    def start_held(b):
        def both(offset):
            for k in range(2):
                direct(b, at(offset, k)).start()

        def last():
            for place in range(PAUSE, half):
                up = chips - chip + place
                pl.when(up < half)(lambda: both(up))

        pl.when(chip >= HOLDERS)(last)

    def tell(step):
        for sign in (1, -1):
            pl.semaphore_signal(
                ready.at[step], inc=1, device_id=dev(at(sign * (NEAR << step), core)), device_id_type=MESH
            )

    def wait_blocks(sem, n):
        ref = own.at[0, :, pl.ds(0, n * pulses)]
        pltpu.make_async_copy(ref, ref, sem).wait()

    inner = (me > 0, me < size - 1)

    def halo_copy(b, side):
        to = lax.rem(me + (1 if side else size - 1), size)
        return pltpu.make_async_remote_copy(
            src_ref=halo_out.at[b, side],
            dst_ref=halo_in.at[b, 1 - side],
            send_sem=hs_sem.at[b, side],
            recv_sem=hr_sem.at[b, 1 - side],
            device_id=dev(to),
            device_id_type=MESH,
        )

    def doppler(b):
        rows = [
            [recv[b, ri, pl.ds(l, size, stride=pulses), :] for l in range(pulses)] for ri in range(2)
        ]
        value = doppler_power(
            rows[0], rows[1], ta[0], lambda l: (dop[0, :, l * GB : (l + 1) * GB], dop[1, :, l * GB : (l + 1) * GB])
        )
        halo_out[b, 0] = pack(value, 0)
        halo_out[b, 1] = pack(value, GB - HALO)
        power[b] = value
        for side in range(2):
            pl.when(inner[side])(halo_copy(b, side).start)

    def cfar_inside(b):
        own_band, left_band, right_band = bands(guard[b], train[b])
        high, low = split(power[b])
        band = own_band.astype(BF16)
        window[b] = jnp.dot(
            jnp.concatenate([high, low], axis=1),
            jnp.concatenate([band, band], axis=0),
            preferred_element_type=F32,
        )
        slot = lax.div(lax.broadcasted_iota(jnp.int32, (GB, GB), 0), 32)
        for r in range(4):
            lb = jnp.where(slot == r, left_band, 0.0).astype(BF16)
            rb = jnp.where(slot == r, right_band, 0.0).astype(BF16)
            edge_band[b, r] = jnp.concatenate([lb, lb, rb, rb], axis=0)

    def cfar(b):
        rows = depth // 4
        for side in range(2):

            def arrived():
                halo_copy(b, side).wait_send()
                halo_copy(b, 1 - side).wait_recv()

            def outside():
                halo_in[b, side] = jnp.zeros_like(halo_in[b, side])

            pl.when(inner[side])(arrived)
            pl.when(jnp.logical_not(inner[side]))(outside)
        left, right = halo_in[b, 0], halo_in[b, 1]
        lh, ll = split(left)
        rh, rl = split(right)
        edges = jnp.concatenate([lh, ll, rh, rl], axis=1)
        floor = noise[b]
        inverse = 1.0 / (2.0 * train[b].astype(F32))
        for r in range(4):
            more = jnp.dot(edges, edge_band[b, r], preferred_element_type=F32)
            here = slice(r * rows, (r + 1) * rows)
            out[0, b, here, :] = power[b, here, :] / (floor + (window[b, here, :] + more) * inverse)

    range_compress(0)
    pl.semaphore_wait(barrier, greeters)
    tell(0)
    direct(0, partner).start()
    start_by_place(0, 1, NEAR)
    start_by_place(0, NEAR + 1, HOP, 0)
    for b in range(1, beams):
        range_compress(b)
    pl.semaphore_wait(ready.at[0], 2)
    tell(1)
    start_by_place(0, NEAR + 1, 2 * NEAR, 1)
    pl.semaphore_wait(ready.at[1], 2)
    tell(2)
    start_by_place(0, 2 * NEAR + 1, HOP, 1)
    pl.semaphore_wait(ready.at[2], 2)
    start_by_place(0, HOP + 1, half)
    for b in range(1, beams):
        direct(b, partner).start()
        start_by_place(b, 1, half, hold=True)
    for b in range(beams):
        keep_own(b)
    for l in range(pulses):
        for i in range(2):
            col = i * pulses + l
            dop[i, :, l * GB : (l + 1) * GB] = jnp.broadcast_to(tw[2, :, col : col + 1], (GA, GB))
    for b in range(beams):
        wait_blocks(recv_sem.at[b], size - 1)
        doppler(b)
        cfar_inside(b)
        if b == 0:
            for other in range(1, beams):
                start_held(other)
    for b in range(beams):
        cfar(b)
    for b in range(beams):
        wait_blocks(own_sem.at[b], size - 1)


def solution(mesh):
    size = mesh.shape["shard"]

    def step(echoes, waveform, taper, guard, train, noise):
        _, _, beams, pulses, gates = echoes.shape
        depth = pulses * size
        tab_a, tab_b, twid = tables(depth)
        hbm = pl.BlockSpec(memory_space=pl.ANY)
        smem = pl.BlockSpec(memory_space=pltpu.SMEM)
        vmem = pltpu.VMEM
        dma = pltpu.SemaphoreType.DMA
        return pl.pallas_call(
            functools.partial(kernel, size),
            out_shape=vmem((1, beams, depth, GB), F32),
            in_specs=[hbm, hbm, smem, smem, smem, smem, hbm, hbm, hbm],
            out_specs=pl.BlockSpec(memory_space=vmem),
            scratch_shapes=[
                vmem((beams, 2, pulses, gates), F32),
                vmem((2, gates), F32),
                vmem(tab_a.shape, BF16),
                vmem(tab_b.shape, BF16),
                vmem(twid.shape, F32),
                vmem((2, GA * pulses, GB), F32),
                vmem((GB, GB), F32),
                vmem((2, GA, GB), F32),
                vmem((beams, 2, depth, GB), F32),
                vmem((beams, 2, depth, GB), F32),
                vmem((2, GA, pulses * GB), F32),
                vmem((beams, depth, GB), F32),
                vmem((beams, depth, GB), F32),
                vmem((beams, 4, 4 * GB, GB), BF16),
                vmem((beams, 2, depth // 4, GB), F32),
                vmem((beams, 2, depth // 4, GB), F32),
                dma((4 + beams,)),
                dma((beams,)),
                dma((beams,)),
                pltpu.SemaphoreType.REGULAR((3,)),
                dma((beams, 2)),
                dma((beams, 2)),
            ],
            compiler_params=pltpu.CompilerParams(
                collective_id=0, has_side_effects=True, vmem_limit_bytes=56 * 2**20
            ),
            name="pulse_doppler",
        )(echoes, waveform, taper, guard, train, noise, jnp.asarray(tab_a), jnp.asarray(tab_b), jnp.asarray(twid))

    in_specs = (
        P(None, None, "groups", "shard", None),
        P(),
        P(),
        P("groups"),
        P("groups"),
        P("groups"),
    )
    out_specs = P(None, "groups", None, "shard")
    return jax.shard_map(step, mesh=mesh, in_specs=in_specs, out_specs=out_specs, check_vma=False)
```
